32 devices in a mesh: rep: 2 (over x), seq: 8 (over z, y), tp: 2 (over core).
Axes of the slice: x: 2, y: 2, z: 4, core: 2. Of those that a mesh axis runs over, the one named last changes fastest.
Arguments:
- prefill_query: bfloat16 [8192, 2048], P(('rep', 'seq'), 'tp'), parts along dimension 0, may hold values from -50 to 50
- prefill_key: bfloat16 [8192, 512], P(('rep', 'seq'), 'tp'), parts along dimension 0, may hold values from -6 to 6
- prefill_value: bfloat16 [8192, 512], P(('rep', 'seq'), 'tp'), parts along dimension 0, may hold values from -6 to 6
- doc_ids: int32 [8192], P('rep'), parts along dimension 0, may hold values from 0 to 3, never falling along the last dimension, each value on 1 to 2048 neighbouring positions
- head_window: int32 [16], P('tp'), may hold values from 1024 to 4096, as said below
- dec_query: bfloat16 [128, 2048], P('rep', 'tp'), parts along dimension 0, may hold values from -50 to 50
- dec_key: bfloat16 [128, 512], P('rep', 'tp'), parts along dimension 0, may hold values from -6 to 6
- dec_value: bfloat16 [128, 512], P('rep', 'tp'), parts along dimension 0, may hold values from -6 to 6
- cache_key: bfloat16 [65536, 512], P(('rep', 'seq'), 'tp'), parts along dimension 0, may hold values from -6 to 6
- cache_value: bfloat16 [65536, 512], P(('rep', 'seq'), 'tp'), parts along dimension 0, may hold values from -6 to 6
- page_order: int32 [512], P(('rep', 'seq')), parts along dimension 0, may hold values from 0 to 255, each once
- lengths: int32 [128], P('rep'), parts along dimension 0, may hold values from 1 to 512, 16384 in all
- out_proj: bfloat16 [2048, 4096], P('tp'), may hold values from -0.125 to 0.125
Outputs:
- prompt_out: bfloat16 [8192, 4096], P(('rep', 'seq', 'tp')), parts along dimension 0
- decode_out: bfloat16 [128, 4096], P(('rep', 'tp')), parts along dimension 0
The draws below stay inside these ranges and needn't reach their ends.
There are 2 independent parts, one for each index of `rep`. The reference program is written for one: setup_inputs(seed, part) draws one part's arguments, and reference() takes and returns one part's arrays. A program takes and returns all parts, laid end to end along the dimension named above; an argument that names none is the same for every part. Nothing has to cross between parts.
Inputs may be any that keep to these rules, and one draw needn't show every extreme that they name: `head_window`: some head has window 4096.
All inputs are finite; a program needn't handle non-finite values.
Results may differ from the reference program's by a relative error of at most 0.015.
Values may be sent and summed in bfloat16 or wider, within the bound.
A program may use at most 256 MiB of HBM per device.

```python
import math
import jax
import jax.numpy as jnp
import numpy as np
from jax import lax

D = 4096
HD = 128
HEADS = 16
KV_HEADS = 4
WINDOW = 4096
REQS = 64
PAGE = 128
TOKENS = 4096
PAGES = 256
MAXLEN = 512
N_TP = 2


def prompt_keys(key):
    base = jax.random.fold_in(key, 7)
    keys = jnp.clip(jax.random.normal(base, (TOKENS, KV_HEADS * HD), jnp.float32), -6.0, 6.0)
    return keys


def draw_prefill_key(key, part):
    return prompt_keys(key).astype(jnp.bfloat16)


def draw_prefill_query(key, part):
    base = jax.random.fold_in(key, 8)
    queries = jnp.clip(jax.random.normal(base, (TOKENS, HEADS * HD), jnp.float32), -6.0, 6.0)
    return queries.astype(jnp.bfloat16)


def decode_keys(key):
    base = jax.random.fold_in(key, 9)
    keys = jnp.clip(jax.random.normal(base, (REQS, KV_HEADS * HD), jnp.float32), -6.0, 6.0)
    return keys


def draw_dec_key(key, part):
    return decode_keys(key).astype(jnp.bfloat16)


def draw_dec_query(key, part):
    base = jax.random.fold_in(key, 10)
    queries = jnp.clip(jax.random.normal(base, (REQS, HEADS * HD), jnp.float32), -6.0, 6.0)
    return queries.astype(jnp.bfloat16)


def draw_head_window(key, part):
    widths = jax.random.randint(jax.random.fold_in(key, 3), (HEADS,), WINDOW // 4, WINDOW + 1)
    picked = jax.random.randint(jax.random.fold_in(key, 4), (), 0, HEADS)
    return jnp.where(jnp.arange(HEADS) == picked, WINDOW, widths).astype(jnp.int32)


def shard_levels(key, shape, split, least, largest):
    factor_of, own = 1.0, jax.random.fold_in(key, 6)
    for dim, parts in split:
        draws = jnp.exp(jax.random.uniform(jax.random.fold_in(own, dim), (parts,), jnp.float32, least / len(split), largest / len(split)))
        factor_of = factor_of * jnp.repeat(draws, shape[dim] // parts).reshape([-1 if axis == dim else 1 for axis in range(len(shape))])
    return factor_of


def length_profile(count, total, most, skew):
    weights = [(1 << 20) // math.isqrt(grade ** skew) + 1 for grade in range(2, count + 1)]
    spare, holding = total - most - (count - 1), [1] * (count - 1)
    while spare > 0:
        free = [i for i in range(count - 1) if holding[i] < most]
        mass, budget = sum([weights[i] for i in free]), spare
        for i in free:
            extra = min(most - holding[i], max(1, budget * weights[i] // mass), spare)
            holding[i] = holding[i] + extra
            spare = spare - extra
    return np.array([most] + holding)


def uneven(stream_key, count, total, bound, lean):
    if count == 2:
        one = jax.random.randint(stream_key, (), max(1, total - bound), min(bound, total - 1) + 1)
        return jnp.stack([one, total - one])
    tallies = jnp.asarray(length_profile(count, total, bound, lean), jnp.int32)
    pairs = (count - 1) // 2
    source_of, taker = tallies[1:1 + 2 * pairs:2], tallies[2:2 + 2 * pairs:2]
    margin = jnp.minimum(source_of - 1, bound - taker)
    passed = jax.random.randint(jax.random.fold_in(stream_key, 1), (pairs,), 0, 1 << 20) % (margin + 1)
    tallies = tallies.at[1:1 + 2 * pairs:2].set(source_of - passed).at[2:2 + 2 * pairs:2].set(taker + passed)
    return tallies[jax.random.permutation(jax.random.fold_in(stream_key, 2), count)]


def normal_values(key, extent, scale, bound, pieces=(), kind=jnp.bfloat16):
    level = shard_levels(key, extent, pieces, -0.22, 0.18) if pieces else 1.0
    entries = jax.random.normal(key, extent, jnp.float32) * scale * level
    return jnp.minimum(jnp.maximum(entries, -bound), bound).astype(kind)


def setup_inputs(seed: int = 0, part: int = 0) -> dict:
    streams_of = jax.random.split(jax.random.key(seed), 14)
    part_keys = jax.random.split(jax.random.fold_in(streams_of[13], part), 14)
    return {
        "prefill_query": draw_prefill_query(jax.random.fold_in(jax.random.fold_in(streams_of[13], part), 71), part),
        "prefill_key": draw_prefill_key(jax.random.fold_in(jax.random.fold_in(streams_of[13], part), 71), part),
        "prefill_value": normal_values(part_keys[2], (TOKENS, KV_HEADS * HD), 1.0, 6.0, ((0, 8), (1, 2))),
        "doc_ids": jnp.searchsorted(jnp.cumsum(uneven(part_keys[3], 4, TOKENS, TOKENS // 2, 1)), jnp.arange(TOKENS), side="right").astype(jnp.int32),
        "head_window": draw_head_window(jax.random.fold_in(streams_of[13], 71), part),
        "dec_query": draw_dec_query(jax.random.fold_in(jax.random.fold_in(streams_of[13], part), 71), part),
        "dec_key": draw_dec_key(jax.random.fold_in(jax.random.fold_in(streams_of[13], part), 71), part),
        "dec_value": normal_values(part_keys[7], (REQS, KV_HEADS * HD), 1.0, 6.0, ((1, 2),)),
        "cache_key": normal_values(part_keys[8], (PAGES * PAGE, KV_HEADS * HD), 1.0, 6.0, ((0, 8), (1, 2))),
        "cache_value": normal_values(part_keys[9], (PAGES * PAGE, KV_HEADS * HD), 1.0, 6.0, ((0, 8), (1, 2))),
        "page_order": jax.random.permutation(part_keys[10], PAGES).astype(jnp.int32),
        "lengths": uneven(part_keys[11], REQS, REQS * MAXLEN // 2, MAXLEN, 2).astype(jnp.int32),
        "out_proj": normal_values(streams_of[12], (HEADS * HD, D), (HEADS * HD) ** -0.5, 0.125, ((0, 2),)),
    }


masked_score = -1e+30

def round_half(values):
    return lax.optimization_barrier(values.astype(jnp.bfloat16)).astype(jnp.float32)

def project(rows_matrix, out_proj):
    columns = HEADS * HD // N_TP
    total = jnp.zeros((rows_matrix.shape[0], D), jnp.float32)
    for group in range(N_TP):
        partial_sum = jnp.dot(rows_matrix[:, group * columns:(group + 1) * columns], out_proj[group * columns:(group + 1) * columns], preferred_element_type=jnp.float32)
        total = total + round_half(partial_sum)
    return total.astype(jnp.bfloat16)

def reference(prefill_query, prefill_key, prefill_value, doc_ids, head_window, dec_query, dec_key, dec_value, cache_key, cache_value, page_order, lengths, out_proj):
    group_size = HEADS // KV_HEADS
    scale_factor = 1.0 / math.sqrt(HD)
    block = math.gcd(512, TOKENS)
    key_pad = jnp.pad(prefill_key, ((WINDOW, 0), (0, 0)))
    value_pad = jnp.pad(prefill_value, ((WINDOW, 0), (0, 0)))
    doc_pad = jnp.pad(doc_ids, (WINDOW, 0), constant_values=-1)
    windows = head_window.reshape(KV_HEADS, group_size)

    def one_block(index):
        start = (index * block).astype(jnp.int32)
        queries = lax.dynamic_slice_in_dim(prefill_query, start, block, 0).reshape(block, KV_HEADS, group_size, HD).astype(jnp.float32)
        keys = lax.dynamic_slice_in_dim(key_pad, start, block + WINDOW, 0).reshape(block + WINDOW, KV_HEADS, HD).astype(jnp.float32)
        values = lax.dynamic_slice_in_dim(value_pad, start, block + WINDOW, 0).reshape(block + WINDOW, KV_HEADS, HD).astype(jnp.float32)
        query_doc = lax.dynamic_slice_in_dim(doc_ids, start, block, 0)
        key_doc = lax.dynamic_slice_in_dim(doc_pad, start, block + WINDOW, 0)
        query_pos = start + jnp.arange(block, dtype=jnp.int32)
        key_pos = start - WINDOW + jnp.arange(block + WINDOW, dtype=jnp.int32)
        gap = query_pos[:, None] - key_pos[None, :]
        allowed = (gap >= 0) & (query_doc[:, None] == key_doc[None, :])
        allowed = allowed[None, None] & (gap[None, None] < windows[:, :, None, None])
        scores = jnp.einsum('tkgd,skd->kgts', queries, keys) * scale_factor
        scores = jnp.where(allowed, scores, masked_score)
        highest = lax.optimization_barrier(jnp.max(scores, axis=-1))
        weights = jnp.where(allowed, jnp.exp(scores - highest[..., None]), 0.0)
        totals = lax.optimization_barrier(jnp.sum(weights, axis=-1))
        output = jnp.einsum('kgts,skd->kgtd', round_half(weights), values) / totals[..., None]
        return output.transpose(2, 0, 1, 3).reshape(block, HEADS * HD).astype(jnp.bfloat16)
    prompt_attn = lax.map(one_block, jnp.arange(TOKENS // block, dtype=jnp.int32)).reshape(TOKENS, HEADS * HD)
    prompt_out = project(prompt_attn, out_proj)
    inverse = jnp.zeros((PAGES,), jnp.int32).at[page_order].set(jnp.arange(PAGES, dtype=jnp.int32))
    cached_keys = cache_key.reshape(PAGES, PAGE, KV_HEADS * HD)[inverse].reshape(REQS, MAXLEN, KV_HEADS, HD).astype(jnp.float32)
    cached_values = cache_value.reshape(PAGES, PAGE, KV_HEADS * HD)[inverse].reshape(REQS, MAXLEN, KV_HEADS, HD).astype(jnp.float32)
    queries = dec_query.reshape(REQS, KV_HEADS, group_size, HD).astype(jnp.float32)
    own_keys = dec_key.reshape(REQS, KV_HEADS, HD).astype(jnp.float32)
    own_values = dec_value.reshape(REQS, KV_HEADS, HD).astype(jnp.float32)
    scores = jnp.einsum('rkgd,rskd->rkgs', queries, cached_keys) * scale_factor
    valid = (jnp.arange(MAXLEN, dtype=jnp.int32)[None, :] < lengths[:, None])[:, None, None, :]
    scores = jnp.where(valid, scores, masked_score)
    own_scores = jnp.einsum('rkgd,rkd->rkg', queries, own_keys) * scale_factor
    highest = jnp.maximum(lax.optimization_barrier(jnp.max(scores, axis=-1)), own_scores)
    weights = jnp.where(valid, jnp.exp(scores - highest[..., None]), 0.0)
    own_weights = jnp.exp(own_scores - highest)
    totals = lax.optimization_barrier(jnp.sum(weights, axis=-1)) + own_weights
    output = jnp.einsum('rkgs,rskd->rkgd', round_half(weights), cached_values) + round_half(own_weights)[..., None] * own_values[:, :, None, :]
    decode_attn = (output / totals[..., None]).reshape(REQS, HEADS * HD).astype(jnp.bfloat16)
    decode_out = project(decode_attn, out_proj)
    return (prompt_out, decode_out)
```

```python
import functools
import math

import jax
import jax.numpy as jnp
from jax import lax
from jax.experimental import pallas as pl
from jax.experimental.pallas import tpu as pltpu
from jax.sharding import PartitionSpec as P

HD = 128
WINDOW = 4096
PAGE = 128
DOCS = 4
MASKED = -1e30
FLOOR = -1e29
NEAR = WINDOW // 4
SUB = 256
SPAN = 2
MESH = pl.DeviceIdType.MESH


def dot_t(a, b):
    return lax.dot_general(a, b, (((1,), (1,)), ((), ())), preferred_element_type=jnp.float32)


def wide(column, width):
    return jnp.concatenate([column] * (width // column.shape[1]), axis=1)


def put(block_p, block_d, out_p, out_d, sem):
    copies = [
        pltpu.make_async_copy(block_p, out_p, sem.at[0]),
        pltpu.make_async_copy(block_d, out_d, sem.at[1]),
    ]
    for copy in copies:
        copy.start()
    for copy in copies:
        copy.wait()


def kernel(
    n, back, reach, pages_request, q_hbm, k_hbm, v_hbm, docs_hbm, windows, order, lengths,
    dq_hbm, dk_hbm, dv_hbm, ck, cv, w,
    out_p, out_d,
    q, k, v, docs, dq, dk, dv,
    kv, top, acc, lo, rows, ckv, cvv, wv, spread, pieces, part, stats, gathered, gathered_stats,
    att, outgoing, incoming,
    local_sem, zs, zr, ys, yr, ps, pr, fs, fr, ts, tr,
):
    me = lax.axis_index("seq")
    core = lax.axis_index("tp")
    other = 1 - core
    odd = lax.rem(me, 2)
    partner = me + 1 - 2 * odd
    tokens = q.shape[0]
    heads = q.shape[1] // HD
    groups = k.shape[1] // HD
    per = heads // groups
    reqs = dq.shape[0]
    pages = order.shape[0]
    owned = heads // SPAN
    scale = 1.0 / math.sqrt(HD)
    exp_scale = scale * math.log2(math.e)

    pairs = (
        (k_hbm, k), (v_hbm, v), (q_hbm, q), (docs_hbm, docs), (dq_hbm, dq), (ck, ckv), (cv, cvv),
        (dk_hbm, dk), (dv_hbm, dv), (w, wv),
    )
    loads = [pltpu.make_async_copy(a, b, local_sem.at[i]) for i, (a, b) in enumerate(pairs)]
    for load in loads:
        load.start()

    barrier = pltpu.get_barrier_semaphore()

    def greet(d, carry):
        pl.semaphore_signal(
            barrier, inc=1, device_id={"seq": lax.rem(me + d, n)}, device_id_type=MESH
        )
        return carry

    lax.fori_loop(1, n, greet, 0)
    pl.semaphore_signal(barrier, inc=1, device_id={"tp": other}, device_id_type=MESH)
    pl.semaphore_wait(barrier, n)

    def source(s, g, i):
        if s == 0:
            return (k, v)[i].at[:, pl.ds(g * HD, HD)]
        return kv.at[s - 1, g, i]

    def along(s, g, i):
        return pltpu.make_async_remote_copy(
            src_ref=source(s, g, i),
            dst_ref=kv.at[s + 1, g, i],
            send_sem=zs.at[s // 2, g, i],
            recv_sem=zr.at[s // 2, g, i],
            device_id={"seq": lax.rem(me + 2, n)},
            device_id_type=MESH,
        )

    def across(s, h, g, i):
        return pltpu.make_async_remote_copy(
            src_ref=source(s, g, i),
            dst_ref=kv.at[2 * h - 2, g, i],
            send_sem=ys.at[h - 1, g, i],
            recv_sem=yr.at[h - 1, g, i],
            device_id={"seq": partner},
            device_id_type=MESH,
        )

    def forward(s, g, finish=False, only=(0, 1)):
        act = (lambda c: c.wait_send()) if finish else (lambda c: c.start())
        if s + 2 <= back:
            @pl.when((me >= s) & (me + 2 < n))
            def _():
                for i in only:
                    act(along(s, g, i))

            @pl.when((me >= s) & (odd == 0))
            def _():
                for i in only:
                    act(across(s, s // 2 + 1, g, i))
        if s >= 2:
            @pl.when((me >= s) & (odd == 1))
            def _():
                for i in only:
                    act(across(s, s // 2, g, i))

    def arrive(s, g):
        @pl.when(me >= s)
        def _():
            for i in range(2):
                if s % 2 == 0:
                    along(s - 2, g, i).wait_recv()
                else:
                    across(s + 1, (s + 1) // 2, g, i).wait_recv()

        if s % 2 == 0:
            forward(s, g)

    def attend(s, g):
        def one_head(head):
            lanes = slice(g * HD, (g + 1) * HD)
            keys = k[:, lanes] if s == 0 else kv[s - 1, g, 0]
            values = v[:, lanes] if s == 0 else kv[s - 1, g, 1]
            values = jnp.concatenate([values, jnp.ones_like(values)], axis=1)
            size = math.gcd(tokens, SUB)
            for r in range(0, tokens, size):
                cut = slice(r, r + size)
                first = max(0, (s * tokens + r - reach + 1) // HD * HD)
                last = r + size if s == 0 else tokens
                span = last - first
                queries = q[cut, head * HD:(head + 1) * HD]
                scores = dot_t(queries, keys[first:last])
                limit = lo[cut]
                if (s + 1) * tokens > NEAR:
                    place = me * tokens + r + lax.broadcasted_iota(jnp.int32, (size, HD), 0)
                    limit = jnp.maximum(limit, place - windows[head] + 1)
                limit = limit - ((me - s) * tokens + first)
                column = lax.broadcasted_iota(jnp.int32, (size, span), 1)
                allowed = column >= wide(limit, span)
                if s == 0:
                    allowed = allowed & (
                        column <= lax.broadcasted_iota(jnp.int32, (size, span), 0) + r
                    )
                scores = jnp.where(allowed, scores, MASKED)
                high = jnp.max(scores, axis=1, keepdims=True) * exp_scale
                high = jnp.broadcast_to(high, (size, HD))
                if s > 0:
                    old = top[head, cut]
                    high = jnp.maximum(high, old)
                weights = jnp.exp2(scores * exp_scale - wide(high, span))
                added = jnp.dot(
                    weights.astype(jnp.bfloat16), values[first:last],
                    preferred_element_type=jnp.float32,
                )
                if s > 0:
                    added = added + acc[head, cut] * wide(jnp.exp2(old - high), 2 * HD)
                top[head, cut] = high
                acc[head, cut] = added

        @pl.when(me >= s)
        def _():
            for r in range(per):
                one_head(g * per + r)

    def to_owner(owner):
        return [
            pltpu.make_async_remote_copy(
                src_ref=src,
                dst_ref=dst.at[me],
                send_sem=ps.at[owner, i],
                recv_sem=pr.at[me, i],
                device_id={"seq": owner},
                device_id_type=MESH,
            )
            for i, (src, dst) in enumerate(
                ((part.at[pl.ds(owner * owned, owned)], gathered), (stats, gathered_stats))
            )
        ]

    def decode_partials():
        for i in (4, 5, 6):
            loads[i].wait()
        spread[...] = jnp.zeros_like(spread)
        for head in range(heads):
            g = head // per
            spread[:, head, g * HD:(g + 1) * HD] = (
                dq[:, head * HD:(head + 1) * HD].astype(jnp.float32)
            )
        step = math.gcd(pages, 8)
        lane = lax.broadcasted_iota(jnp.int32, (heads, PAGE), 1)
        group = lax.broadcasted_iota(jnp.int32, (heads, HD), 0) // per

        def block(b, carry):
            levels, owners = carry
            scores, spans, who = [], [], []
            for i in range(step):
                page = order[b * step + i]
                owner = page // pages_request
                left = lengths[owner] - (page - owner * pages_request) * PAGE
                span = pl.ds(pl.multiple_of((b * step + i) * PAGE, PAGE), PAGE)
                score = dot_t(spread[owner].astype(jnp.bfloat16), ckv[span, :])
                scores.append(jnp.where(lane < left, score, MASKED))
                spans.append(span)
                who.append(owner)
            scores = jnp.concatenate(scores, axis=0)
            high = jnp.max(scores, axis=1, keepdims=True)
            high = jnp.broadcast_to(jnp.maximum(high, FLOOR) * exp_scale, scores.shape)
            weights = jnp.exp2(scores * exp_scale - high)
            total = jnp.broadcast_to(jnp.sum(weights, axis=1, keepdims=True), scores.shape)
            some = total > 0.0
            whole = jnp.where(some, total, 1.0)
            level = jnp.where(some, high + jnp.log2(whole), FLOOR)
            weights = (weights / whole).astype(jnp.bfloat16)
            for i in range(step):
                cut = slice(i * heads, (i + 1) * heads)
                both = jnp.dot(
                    weights[cut], cvv[spans[i], :], preferred_element_type=jnp.float32
                )
                mixed = both[:, :HD]
                for g in range(1, groups):
                    mixed = jnp.where(group == g, both[:, g * HD:(g + 1) * HD], mixed)
                pieces[b * step + i] = mixed
                here = lane == b * step + i
                levels = jnp.where(here, level[cut], levels)
                owners = jnp.where(here, who[i].astype(jnp.float32), owners)
            return (levels, owners)

        blank = jnp.zeros((heads, PAGE), jnp.float32)
        levels, owners = lax.fori_loop(
            0, pages // step, block, (blank + FLOOR, blank - 1.0)
        )
        stats[:heads] = levels
        stats[heads:] = owners
        for head in range(heads):
            part[head] = pieces[:, head].astype(jnp.bfloat16)
        for owner in range(SPAN):
            @pl.when(me != owner)
            def _():
                for copy in to_owner(owner):
                    copy.start()

    def decode_merge():
        @pl.when(me < SPAN)
        def _():
            loads[7].wait()
            loads[8].wait()
            gathered[me] = part[pl.ds(me * owned, owned)]
            gathered_stats[me] = stats[...]

            def take(d, carry):
                j = lax.rem(me + d, n)
                for i, (src, dst) in enumerate(
                    ((part.at[pl.ds(0, owned)], gathered), (stats, gathered_stats))
                ):
                    pltpu.make_async_remote_copy(
                        src_ref=src,
                        dst_ref=dst.at[j],
                        send_sem=ps.at[0, i],
                        recv_sem=pr.at[j, i],
                        device_id={"seq": partner},
                        device_id_type=MESH,
                    ).wait_recv()
                return carry

            lax.fori_loop(1, n, take, 0)
            request = lax.broadcasted_iota(jnp.int32, (reqs, PAGE), 0).astype(jnp.float32)

            def one_head(r, carry):
                head = me * owned + r
                queries = dq[:, pl.ds(pl.multiple_of(head * HD, HD), HD)].astype(jnp.float32)
                group = pl.ds(pl.multiple_of((head // per) * HD, HD), HD)
                own = jnp.sum(queries * dk[:, group].astype(jnp.float32), axis=1, keepdims=True)
                own = jnp.broadcast_to(own * exp_scale, (reqs, HD))
                levels = []
                high = own
                for j in range(n):
                    level = gathered_stats[j, pl.ds(head, 1), :]
                    level = jnp.where(gathered_stats[j, heads:heads + 1, :] == request, level, FLOOR)
                    levels.append(level)
                    high = jnp.maximum(
                        high, jnp.broadcast_to(jnp.max(level, axis=1, keepdims=True), high.shape)
                    )
                mine = jnp.exp2(own - high)
                summed = mine * dv[:, group].astype(jnp.float32)
                total = jnp.zeros((reqs, PAGE), jnp.float32)
                for j in range(n):
                    weight = jnp.exp2(levels[j] - high)
                    total = total + weight
                    summed = summed + jnp.dot(
                        weight[:, :pages].astype(jnp.bfloat16), gathered[j, r],
                        preferred_element_type=jnp.float32,
                    )
                total = mine + jnp.broadcast_to(
                    jnp.sum(total, axis=1, keepdims=True), mine.shape
                )
                att[head] = (summed / total).astype(jnp.bfloat16)
                return carry

            lax.fori_loop(0, owned, one_head, 0)

    def finals(i, half=None):
        half = pl.ds((odd if half is None else half) * owned, owned)
        return pltpu.make_async_remote_copy(
            src_ref=att.at[half],
            dst_ref=att.at[half],
            send_sem=fs.at[i],
            recv_sem=fr.at[i],
            device_id={"seq": partner if i else lax.rem(me + 2, n)},
            device_id_type=MESH,
        )

    def relay(level):
        @pl.when(me // SPAN == level)
        def _():
            if level:
                finals(0).wait_recv()

            @pl.when(me + 2 < n)
            def _():
                finals(0).start()

            finals(1).start()

    for i in (0, 1):
        loads[i].wait()
    for g in range(groups):
        forward(0, g)
    loads[3].wait()
    position = me * tokens + lax.broadcasted_iota(jnp.int32, (tokens, HD), 0)
    place = position.astype(jnp.float32)
    start = jnp.zeros((tokens, HD), jnp.float32)
    for document in range(1, DOCS):
        before = (docs[...] < document).astype(jnp.float32)
        before = jnp.sum(jnp.sum(before, axis=0, keepdims=True), axis=1, keepdims=True)
        start = jnp.where(before <= place, jnp.maximum(start, before), start)
    lo[...] = start.astype(jnp.int32)
    decode_partials()
    loads[2].wait()
    for g in range(groups):
        attend(0, g)
    for g in range(groups):
        arrive(2, g)
        attend(2, g)
    decode_merge()
    relay(0)
    relay(1)
    levels = n // SPAN
    for h in range(1, back // 2 + 1):
        for g in range(groups):
            if 2 * h + 2 <= back:
                arrive(2 * h + 2, g)
            arrive(2 * h - 1, g)
            attend(2 * h - 1, g)
            if h == 1 and g == 0 and levels > 2:
                relay(2)
            if h == 1 and g == groups - 1:
                for level in range(3, levels):
                    relay(level)
        if 2 * h + 2 <= back:
            for g in range(groups):
                attend(2 * h + 2, g)

    half = tokens // 2
    half_reqs = reqs // 2
    finals(1, 1 - odd).wait_recv()
    for head in range(heads):
        cut = slice(head * HD, (head + 1) * HD)
        done = (acc[head, :, :HD] / acc[head, :, HD:]).astype(jnp.bfloat16)
        for c in range(2):
            rows[c, :half, cut] = done[c * half:(c + 1) * half]
            rows[c, half:, cut] = att[head, c * half_reqs:(c + 1) * half_reqs]

    loads[9].wait()
    blocks = outgoing.shape[0]
    width = outgoing.shape[2]

    def exchange(b):
        return pltpu.make_async_remote_copy(
            src_ref=outgoing.at[b],
            dst_ref=incoming.at[b],
            send_sem=ts.at[b],
            recv_sem=tr.at[b],
            device_id={"tp": other},
            device_id_type=MESH,
        )

    def project(c, b):
        span = pl.ds(pl.multiple_of(b * width, width), width)
        return jnp.dot(rows[c], wv[:, span], preferred_element_type=jnp.float32)

    def give(b, carry):
        outgoing[b] = project(other, b).astype(jnp.bfloat16)
        exchange(b).start()
        return carry

    def keep(b, carry):
        own = project(core, b).astype(jnp.bfloat16).astype(jnp.float32)
        exchange(b).wait_recv()
        total = (own + incoming[b].astype(jnp.float32)).astype(jnp.bfloat16)
        span = pl.ds(pl.multiple_of(b * width, width), width)
        out_p[:, span] = total[:half]
        out_d[:, span] = total[half:]
        return carry

    lax.fori_loop(0, blocks, give, 0)
    lax.fori_loop(0, blocks, keep, 0)

    def sent(b, carry):
        exchange(b).wait_send()
        return carry

    lax.fori_loop(0, blocks, sent, 0)
    for s in range(0, back + 1, 2):
        for g in range(groups):
            forward(s, g, finish=True)
    for owner in range(SPAN):
        @pl.when(me != owner)
        def _():
            for copy in to_owner(owner):
                copy.wait_send()

    @pl.when(me + 2 < n)
    def _():
        finals(0).wait_send()

    finals(1).wait_send()

    @pl.when(me >= SPAN)
    def _():
        loads[7].wait()
        loads[8].wait()


def on_device(
    n, prefill_query, prefill_key, prefill_value, doc_ids, head_window, dec_query, dec_key,
    dec_value, cache_key, cache_value, page_order, lengths, out_proj,
):
    tokens, width = prefill_query.shape
    heads = width // HD
    groups = prefill_key.shape[1] // HD
    reqs = dec_query.shape[0]
    model = out_proj.shape[1]
    pages = page_order.shape[0]
    reach = min(doc_ids.shape[0] // 2, WINDOW)
    back = -(-reach // tokens)
    back += back % 2

    pages_request = page_order.shape[0] * n // reqs
    docs = doc_ids.reshape(-1, HD)
    vmem = pl.BlockSpec(memory_space=pltpu.VMEM)
    hbm = pl.BlockSpec(memory_space=pltpu.HBM)
    smem = pl.BlockSpec(memory_space=pltpu.SMEM)
    block = 512
    blocks = model // block
    merged = (tokens + reqs) // 2
    dma = pltpu.SemaphoreType.DMA
    args = (
        prefill_query, prefill_key, prefill_value, docs, head_window, page_order, lengths,
        dec_query, dec_key, dec_value, cache_key, cache_value, out_proj,
    )
    result = pl.pallas_call(
        functools.partial(kernel, n, back, reach, pages_request),
        out_shape=(
            jax.ShapeDtypeStruct((tokens // 2, model), jnp.bfloat16),
            jax.ShapeDtypeStruct((reqs // 2, model), jnp.bfloat16),
        ),
        in_specs=[hbm] * 4 + [smem] * 3 + [hbm] * 6,
        out_specs=(vmem, vmem),
        scratch_shapes=[
            pltpu.VMEM(prefill_query.shape, jnp.bfloat16),
            pltpu.VMEM(prefill_key.shape, jnp.bfloat16),
            pltpu.VMEM(prefill_value.shape, jnp.bfloat16),
            pltpu.VMEM(docs.shape, jnp.int32),
            pltpu.VMEM(dec_query.shape, jnp.bfloat16),
            pltpu.VMEM(dec_key.shape, jnp.bfloat16),
            pltpu.VMEM(dec_value.shape, jnp.bfloat16),
            pltpu.VMEM((back, groups, 2, tokens, HD), jnp.bfloat16),
            pltpu.VMEM((heads, tokens, HD), jnp.float32),
            pltpu.VMEM((heads, tokens, 2 * HD), jnp.float32),
            pltpu.VMEM((tokens, HD), jnp.int32),
            pltpu.VMEM((2, merged, heads * HD), jnp.bfloat16),
            pltpu.VMEM(cache_key.shape, jnp.bfloat16),
            pltpu.VMEM(cache_value.shape, jnp.bfloat16),
            pltpu.VMEM(out_proj.shape, jnp.bfloat16),
            pltpu.VMEM((reqs, heads, groups * HD), jnp.float32),
            pltpu.VMEM((pages, heads, HD), jnp.float32),
            pltpu.VMEM((heads, pages, HD), jnp.bfloat16),
            pltpu.VMEM((2 * heads, PAGE), jnp.float32),
            pltpu.VMEM((n, heads // SPAN, pages, HD), jnp.bfloat16),
            pltpu.VMEM((n, 2 * heads, PAGE), jnp.float32),
            pltpu.VMEM((heads, reqs, HD), jnp.bfloat16),
            pltpu.VMEM((blocks, merged, block), jnp.bfloat16),
            pltpu.VMEM((blocks, merged, block), jnp.bfloat16),
            dma((10,)),
            dma((back // 2, groups, 2)),
            dma((back // 2, groups, 2)),
            dma((back // 2, groups, 2)),
            dma((back // 2, groups, 2)),
            dma((SPAN, 2)),
            dma((n, 2)),
            dma((2,)),
            dma((2,)),
            dma((blocks,)),
            dma((blocks,)),
        ],
        compiler_params=pltpu.CompilerParams(
            collective_id=0, has_side_effects=True, vmem_limit_bytes=48 * 1024 * 1024
        ),
    )(*[pltpu.with_memory_space_constraint(x, pltpu.HBM) for x in args])
    return pl.pallas_call(
        put,
        out_shape=tuple(jax.ShapeDtypeStruct(x.shape, x.dtype) for x in result),
        in_specs=[vmem, vmem],
        out_specs=(hbm, hbm),
        scratch_shapes=[dma((2,))],
        compiler_params=pltpu.CompilerParams(vmem_limit_bytes=4 * 1024 * 1024),
    )(*result)


def solution(mesh):
    placed = (
        P(("rep", "seq"), "tp"),
        P(("rep", "seq"), "tp"),
        P(("rep", "seq"), "tp"),
        P("rep"),
        P("tp"),
        P("rep", "tp"),
        P("rep", "tp"),
        P("rep", "tp"),
        P(("rep", "seq"), "tp"),
        P(("rep", "seq"), "tp"),
        P(("rep", "seq")),
        P("rep"),
        P("tp", None),
    )
    return jax.shard_map(
        functools.partial(on_device, mesh.shape["seq"]),
        mesh=mesh,
        in_specs=placed,
        out_specs=(P(("rep", "seq", "tp"), None), P(("rep", "tp"), None)),
        check_vma=False,
    )
```

```python
import functools
import math

import jax
import jax.numpy as jnp
from jax import lax
from jax.experimental import pallas as pl
from jax.experimental.pallas import tpu as pltpu
from jax.sharding import PartitionSpec as P

HD = 128
WINDOW = 4096
PAGE = 128
DOCS = 4
MASKED = -1e30
FLOOR = -1e29
NEAR = WINDOW // 4
SUB = 256
CUTS = 2
MESH = pl.DeviceIdType.MESH


def dot_t(a, b):
    return lax.dot_general(a, b, (((1,), (1,)), ((), ())), preferred_element_type=jnp.float32)


def wide(column, width):
    return jnp.concatenate([column] * (width // column.shape[1]), axis=1)


def put(block_p, block_d, out_p, out_d, sem):
    copies = [
        pltpu.make_async_copy(block_p, out_p, sem.at[0]),
        pltpu.make_async_copy(block_d, out_d, sem.at[1]),
    ]
    for copy in copies:
        copy.start()
    for copy in copies:
        copy.wait()


def kernel(
    n, back, reach, pages_request, q_hbm, k_hbm, v_hbm, docs_hbm, windows, order, lengths,
    dq_hbm, dk_hbm, dv_hbm, ck, cv, w,
    out_p, out_d,
    q, k, v, docs, dq, dk, dv,
    kv, top, acc, lo, rows, ckv, cvv, wv, spread, pieces, part, stats, gathered, gathered_stats,
    att, total, wx, incoming,
    local_sem, zs, zr, ys, yr, ps, pr, fs, fr, ts, tr, ws, wr, gate,
):
    me = lax.axis_index("seq")
    core = lax.axis_index("tp")
    other = 1 - core
    odd = lax.rem(me, 2)
    partner = me + 1 - 2 * odd
    tokens = q.shape[0]
    heads = q.shape[1] // HD
    groups = k.shape[1] // HD
    per = heads // groups
    reqs = dq.shape[0]
    pages = order.shape[0]
    scale = 1.0 / math.sqrt(HD)
    exp_scale = scale * math.log2(math.e)

    pairs = (
        (k_hbm, k), (v_hbm, v), (dq_hbm, dq), (ck, ckv), (cv, cvv), (docs_hbm, docs), (q_hbm, q),
        (dk_hbm, dk), (dv_hbm, dv), (w, wv),
    )
    loads = [pltpu.make_async_copy(a, b, local_sem.at[i]) for i, (a, b) in enumerate(pairs)]
    for load in loads[:7]:
        load.start()

    barrier = pltpu.get_barrier_semaphore()

    @pl.when(me >= 2)
    def _():
        pl.semaphore_signal(barrier, inc=1, device_id={"seq": me - 2}, device_id_type=MESH)

    pl.semaphore_signal(barrier, inc=1, device_id={"seq": partner}, device_id_type=MESH)
    pl.semaphore_signal(barrier, inc=1, device_id={"tp": other}, device_id_type=MESH)
    pl.semaphore_wait(barrier, 2 + (me + 2 < n).astype(jnp.int32))

    def pass_gate():
        @pl.when(me >= 2)
        def _():
            pl.semaphore_wait(gate, 1)

        @pl.when(me + 2 < n)
        def _():
            pl.semaphore_signal(gate, inc=1, device_id={"seq": me + 2}, device_id_type=MESH)

    piece = tokens // CUTS

    def source(s, g, i, c):
        span = pl.ds(c * piece, piece)
        if s == 0:
            return (k, v)[i].at[span, pl.ds(g * HD, HD)]
        return kv.at[s - 1, g, i, span]

    def along(s, g, i, c):
        return pltpu.make_async_remote_copy(
            src_ref=source(s, g, i, c),
            dst_ref=kv.at[s + 1, g, i, pl.ds(c * piece, piece)],
            send_sem=zs.at[s // 2, g, i, c],
            recv_sem=zr.at[s // 2, g, i, c],
            device_id={"seq": lax.rem(me + 2, n)},
            device_id_type=MESH,
        )

    def across(s, h, g, i, c):
        return pltpu.make_async_remote_copy(
            src_ref=source(s, g, i, c),
            dst_ref=kv.at[2 * h - 2, g, i, pl.ds(c * piece, piece)],
            send_sem=ys.at[h - 1, g, i, c],
            recv_sem=yr.at[h - 1, g, i, c],
            device_id={"seq": partner},
            device_id_type=MESH,
        )

    def forward(s, g, finish=False, only=tuple((i, c) for c in range(CUTS) for i in range(2))):
        act = (lambda c: c.wait_send()) if finish else (lambda c: c.start())
        if s + 2 <= back:
            @pl.when((me >= s) & (me + 2 < n))
            def _():
                for i, c in only:
                    act(along(s, g, i, c))

            @pl.when((me >= s) & (odd == 0))
            def _():
                for i, c in only:
                    act(across(s, s // 2 + 1, g, i, c))
        if s >= 2:
            @pl.when((me >= s) & (odd == 1))
            def _():
                for i, c in only:
                    act(across(s, s // 2, g, i, c))

    order_of = tuple((i, c) for c in range(CUTS) for i in range(2))

    def arrive(s, g, only=order_of):
        for i, c in only:
            @pl.when(me >= s)
            def _():
                if s % 2 == 0:
                    along(s - 2, g, i, c).wait_recv()
                else:
                    across(s + 1, (s + 1) // 2, g, i, c).wait_recv()

            if s % 2 == 0:
                forward(s, g, only=((i, c),))

    def attend(s, g, low=0, top_key=None):
        def one_head(head):
            lanes = slice(g * HD, (g + 1) * HD)
            size = math.gcd(tokens, SUB)
            for r in range(0, tokens, size):
                cut = slice(r, r + size)
                first = max(low, (s * tokens + r - reach + 1) // HD * HD)
                last = min(r + size if s == 0 else tokens, top_key or tokens)
                if first >= last:
                    continue
                span = last - first
                queries = q[cut, head * HD:(head + 1) * HD]
                part_of = slice(first, last)
                keys = k[part_of, lanes] if s == 0 else kv[s - 1, g, 0, part_of]
                values = v[part_of, lanes] if s == 0 else kv[s - 1, g, 1, part_of]
                values = jnp.concatenate([values, jnp.ones_like(values)], axis=1)
                scores = dot_t(queries, keys)
                limit = lo[cut]
                if (s + 1) * tokens > NEAR:
                    place = me * tokens + r + lax.broadcasted_iota(jnp.int32, (size, HD), 0)
                    limit = jnp.maximum(limit, place - windows[head] + 1)
                limit = limit - ((me - s) * tokens + first)
                column = lax.broadcasted_iota(jnp.int32, (size, span), 1)
                allowed = column >= wide(limit, span)
                if s == 0:
                    allowed = allowed & (
                        column <= lax.broadcasted_iota(jnp.int32, (size, span), 0) + r
                    )
                scores = jnp.where(allowed, scores, MASKED)
                high = jnp.max(scores, axis=1, keepdims=True) * exp_scale
                high = jnp.broadcast_to(high, (size, HD))
                if s > 0:
                    old = top[head, cut]
                    high = jnp.maximum(high, old)
                weights = jnp.exp2(scores * exp_scale - wide(high, span))
                added = jnp.dot(
                    weights.astype(jnp.bfloat16), values,
                    preferred_element_type=jnp.float32,
                )
                if s > 0:
                    added = added + acc[head, cut] * wide(jnp.exp2(old - high), 2 * HD)
                top[head, cut] = high
                acc[head, cut] = added

        @pl.when(me >= s)
        def _():
            for r in range(per):
                one_head(g * per + r)

    def to_owner(j):
        return [
            pltpu.make_async_remote_copy(
                src_ref=src,
                dst_ref=dst.at[j],
                send_sem=ps.at[i],
                recv_sem=pr.at[j, i],
                device_id={"seq": 0},
                device_id_type=MESH,
            )
            for i, (src, dst) in enumerate(((part, gathered), (stats, gathered_stats)))
        ]

    def decode_partials():
        for i in (2, 3, 4):
            loads[i].wait()
        spread[...] = jnp.zeros_like(spread)
        for head in range(heads):
            g = head // per
            spread[:, head, g * HD:(g + 1) * HD] = (
                dq[:, head * HD:(head + 1) * HD].astype(jnp.float32)
            )
        step = math.gcd(pages, 8)
        lane = lax.broadcasted_iota(jnp.int32, (heads, PAGE), 1)
        group = lax.broadcasted_iota(jnp.int32, (heads, HD), 0) // per

        def block(b, carry):
            levels, owners = carry
            scores, spans, who = [], [], []
            for i in range(step):
                page = order[b * step + i]
                owner = page // pages_request
                left = lengths[owner] - (page - owner * pages_request) * PAGE
                span = pl.ds(pl.multiple_of((b * step + i) * PAGE, PAGE), PAGE)
                score = dot_t(spread[owner].astype(jnp.bfloat16), ckv[span, :])
                scores.append(jnp.where(lane < left, score, MASKED))
                spans.append(span)
                who.append(owner)
            scores = jnp.concatenate(scores, axis=0)
            high = jnp.max(scores, axis=1, keepdims=True)
            high = jnp.broadcast_to(jnp.maximum(high, FLOOR) * exp_scale, scores.shape)
            weights = jnp.exp2(scores * exp_scale - high)
            total = jnp.broadcast_to(jnp.sum(weights, axis=1, keepdims=True), scores.shape)
            some = total > 0.0
            whole = jnp.where(some, total, 1.0)
            level = jnp.where(some, high + jnp.log2(whole), FLOOR)
            weights = (weights / whole).astype(jnp.bfloat16)
            for i in range(step):
                cut = slice(i * heads, (i + 1) * heads)
                both = jnp.dot(
                    weights[cut], cvv[spans[i], :], preferred_element_type=jnp.float32
                )
                mixed = both[:, :HD]
                for g in range(1, groups):
                    mixed = jnp.where(group == g, both[:, g * HD:(g + 1) * HD], mixed)
                pieces[b * step + i] = mixed
                here = lane == b * step + i
                levels = jnp.where(here, level[cut], levels)
                owners = jnp.where(here, who[i].astype(jnp.float32), owners)
            return (levels, owners)

        blank = jnp.zeros((heads, PAGE), jnp.float32)
        levels, owners = lax.fori_loop(
            0, pages // step, block, (blank + FLOOR, blank - 1.0)
        )
        stats[:heads] = levels
        stats[heads:] = owners
        for head in range(heads):
            part[head] = pieces[:, head].astype(jnp.bfloat16)

        @pl.when(me > 0)
        def _():
            for copy in to_owner(me):
                copy.start()

    def decode_merge():
        @pl.when(me == 0)
        def _():
            loads[7].wait()
            loads[8].wait()
            gathered[0] = part[...]
            gathered_stats[0] = stats[...]
            for j in range(1, n):
                for copy in to_owner(j):
                    copy.wait_recv()
            request = lax.broadcasted_iota(jnp.int32, (reqs, PAGE), 0).astype(jnp.float32)

            def one_head(r):
                queries = dq[:, r * HD:(r + 1) * HD].astype(jnp.float32)
                group = slice(r // per * HD, (r // per + 1) * HD)
                own = jnp.sum(queries * dk[:, group].astype(jnp.float32), axis=1, keepdims=True)
                own = jnp.broadcast_to(own * exp_scale, (reqs, HD))
                levels = [
                    jnp.where(
                        gathered_stats[j, heads:heads + 1, :] == request,
                        gathered_stats[j, r:r + 1, :], FLOOR,
                    )
                    for j in range(n)
                ]
                high = functools.reduce(jnp.maximum, levels)
                high = jnp.broadcast_to(jnp.max(high, axis=1, keepdims=True), own.shape)
                high = jnp.maximum(own, high)
                mine = jnp.exp2(own - high)
                weights = [jnp.exp2(level - high) for level in levels]
                count = jnp.sum(sum(weights), axis=1, keepdims=True)
                summed = mine * dv[:, group].astype(jnp.float32)
                for j in range(n):
                    summed = summed + jnp.dot(
                        weights[j][:, :pages].astype(jnp.bfloat16), gathered[j, r],
                        preferred_element_type=jnp.float32,
                    )
                att[r] = (summed / (mine + count)).astype(jnp.bfloat16)

            for r in range(heads):
                one_head(r)

    levels = n // 2
    near = max(levels // 2, 1)

    def finals(level):
        return pltpu.make_async_remote_copy(
            src_ref=att,
            dst_ref=att,
            send_sem=fs.at[level],
            recv_sem=fr.at[0 if level else 1],
            device_id={"seq": 2 * level if level else partner},
            device_id_type=MESH,
        )

    def publish(finish=False):
        act = (lambda c: c.wait_send()) if finish else (lambda c: c.start())

        @pl.when(me == 0)
        def _():
            for level in range(min(near, levels - 1), 0, -1):
                act(finals(level))

    def relay(finish=False):
        act = (lambda c: c.wait_send()) if finish else (lambda c: c.start())
        for level in range(near + 1, levels):
            @pl.when(me == 2 * (level - near + 1))
            def _():
                if not finish:
                    finals(1).wait_recv()
                act(finals(level))

    def share(finish=False):
        relays = range(2, levels - near + 1)

        @pl.when(odd == 0)
        def _():
            if finish:
                finals(0).wait_send()
            else:
                waiting = me >= 2
                for level in relays:
                    waiting = waiting & (me != 2 * level)

                @pl.when(waiting)
                def _():
                    finals(1).wait_recv()

                finals(0).start()

    half = tokens // 2
    half_reqs = reqs // 2
    wide_rows = per * HD
    width = total.shape[2]
    blocks = total.shape[0]

    def borrow(g):
        span = pl.ds(g * wide_rows, wide_rows)
        return pltpu.make_async_remote_copy(
            src_ref=w.at[span],
            dst_ref=wx.at[span],
            send_sem=ws.at[g],
            recv_sem=wr.at[g],
            device_id={"tp": other},
            device_id_type=MESH,
        )

    def exchange(g):
        return pltpu.make_async_remote_copy(
            src_ref=rows.at[g, other],
            dst_ref=incoming.at[g],
            send_sem=ts.at[g],
            recv_sem=tr.at[g],
            device_id={"tp": other},
            device_id_type=MESH,
        )

    def settle(g):
        for r in range(per):
            head = g * per + r
            cut = slice(r * HD, (r + 1) * HD)
            done = (acc[head, :, :HD] / acc[head, :, HD:]).astype(jnp.bfloat16)
            for c in range(2):
                rows[g, c, :half, cut] = done[c * half:(c + 1) * half]
                rows[g, c, half:, cut] = att[head, c * half_reqs:(c + 1) * half_reqs]
        exchange(g).start()

    def project(g, mine):
        weights = wv if mine else wx
        depth = slice(g * wide_rows, (g + 1) * wide_rows)
        first = mine and g == 0
        last = not mine and g == groups - 1

        def block(b, carry):
            span = pl.ds(pl.multiple_of(b * width, width), width)
            left = rows[g, core] if mine else incoming[g]
            added = jnp.dot(left, weights[depth, span], preferred_element_type=jnp.float32)
            if not first:
                added = added + total[b]
            if last:
                out_p[:, span] = added[:half].astype(jnp.bfloat16)
                out_d[:, span] = added[half:].astype(jnp.bfloat16)
            else:
                total[b] = added
            return carry

        lax.fori_loop(0, blocks, block, 0)

    for i in (0, 1):
        loads[i].wait()
    for g in range(groups):
        forward(0, g)
    pass_gate()
    decode_partials()
    for load in loads[7:]:
        load.start()
    for g in range(groups):
        borrow(g).start()
    loads[5].wait()
    position = me * tokens + lax.broadcasted_iota(jnp.int32, (tokens, HD), 0)
    place = position.astype(jnp.float32)
    start = jnp.zeros((tokens, HD), jnp.float32)
    for document in range(1, DOCS):
        before = (docs[...] < document).astype(jnp.float32)
        before = jnp.sum(jnp.sum(before, axis=0, keepdims=True), axis=1, keepdims=True)
        start = jnp.where(before <= place, jnp.maximum(start, before), start)
    lo[...] = start.astype(jnp.int32)
    loads[6].wait()
    steps = [(s, g) for s in range(2, back + 1, 2) for g in range(groups)]
    arrive(*steps[0], order_of[:1])
    for g in range(groups):
        attend(0, g)
        if g == 0:
            arrive(*steps[0], order_of[1:2])
    decode_merge()
    publish()

    def early():
        @pl.when(odd == 1)
        def _():
            finals(0).wait_recv()

        settle(0)
        loads[9].wait()
        project(0, True)
        for i in range(groups):
            borrow(i).wait_recv()
        exchange(0).wait_recv()
        if groups > 1:
            project(0, False)

    for step, (s, g) in enumerate(steps):
        later = steps[step + 1:step + 2]
        arrive(s, g, order_of[2:])
        attend(s, g)
        for following in later:
            arrive(*following, order_of[:1])
        if not later:
            pl.when(odd == 0)(early)
            for c in range(CUTS):
                arrive(s - 1, g, order_of[2 * c:2 * c + 2])
                attend(s - 1, g, c * piece, (c + 1) * piece)
            pl.when(odd == 1)(early)
        else:
            arrive(s - 1, g)
            attend(s - 1, g)
        for following in later:
            arrive(*following, order_of[1:2])
        if s == 2 and g == groups - 1:
            relay()
        if s == back and g == 0:
            share()
    for g in range(1, groups):
        settle(g)
        project(g, True)
        exchange(g).wait_recv()
        if g < groups - 1:
            project(g, False)
    project(groups - 1, False)

    for g in range(groups):
        exchange(g).wait_send()
        borrow(g).wait_send()
    for s in range(0, back + 1, 2):
        for g in range(groups):
            forward(s, g, finish=True)
    @pl.when(me > 0)
    def _():
        for copy in to_owner(me):
            copy.wait_send()
        loads[7].wait()
        loads[8].wait()

    publish(True)
    relay(True)
    share(True)


def on_device(
    n, prefill_query, prefill_key, prefill_value, doc_ids, head_window, dec_query, dec_key,
    dec_value, cache_key, cache_value, page_order, lengths, out_proj,
):
    tokens, width = prefill_query.shape
    heads = width // HD
    groups = prefill_key.shape[1] // HD
    reqs = dec_query.shape[0]
    model = out_proj.shape[1]
    pages = page_order.shape[0]
    reach = min(doc_ids.shape[0] // 2, WINDOW)
    back = -(-reach // tokens)
    back += back % 2

    pages_request = page_order.shape[0] * n // reqs
    docs = doc_ids.reshape(-1, HD)
    vmem = pl.BlockSpec(memory_space=pltpu.VMEM)
    hbm = pl.BlockSpec(memory_space=pltpu.HBM)
    smem = pl.BlockSpec(memory_space=pltpu.SMEM)
    block = 1024
    blocks = model // block
    merged = (tokens + reqs) // 2
    dma = pltpu.SemaphoreType.DMA
    args = (
        prefill_query, prefill_key, prefill_value, docs, head_window, page_order, lengths,
        dec_query, dec_key, dec_value, cache_key, cache_value, out_proj,
    )
    result = pl.pallas_call(
        functools.partial(kernel, n, back, reach, pages_request),
        out_shape=(
            jax.ShapeDtypeStruct((tokens // 2, model), jnp.bfloat16),
            jax.ShapeDtypeStruct((reqs // 2, model), jnp.bfloat16),
        ),
        in_specs=[hbm] * 4 + [smem] * 3 + [hbm] * 6,
        out_specs=(vmem, vmem),
        scratch_shapes=[
            pltpu.VMEM(prefill_query.shape, jnp.bfloat16),
            pltpu.VMEM(prefill_key.shape, jnp.bfloat16),
            pltpu.VMEM(prefill_value.shape, jnp.bfloat16),
            pltpu.VMEM(docs.shape, jnp.int32),
            pltpu.VMEM(dec_query.shape, jnp.bfloat16),
            pltpu.VMEM(dec_key.shape, jnp.bfloat16),
            pltpu.VMEM(dec_value.shape, jnp.bfloat16),
            pltpu.VMEM((back, groups, 2, tokens, HD), jnp.bfloat16),
            pltpu.VMEM((heads, tokens, HD), jnp.float32),
            pltpu.VMEM((heads, tokens, 2 * HD), jnp.float32),
            pltpu.VMEM((tokens, HD), jnp.int32),
            pltpu.VMEM((groups, 2, merged, heads // groups * HD), jnp.bfloat16),
            pltpu.VMEM(cache_key.shape, jnp.bfloat16),
            pltpu.VMEM(cache_value.shape, jnp.bfloat16),
            pltpu.VMEM(out_proj.shape, jnp.bfloat16),
            pltpu.VMEM((reqs, heads, groups * HD), jnp.float32),
            pltpu.VMEM((pages, heads, HD), jnp.float32),
            pltpu.VMEM((heads, pages, HD), jnp.bfloat16),
            pltpu.VMEM((2 * heads, PAGE), jnp.float32),
            pltpu.VMEM((n, heads, pages, HD), jnp.bfloat16),
            pltpu.VMEM((n, 2 * heads, PAGE), jnp.float32),
            pltpu.VMEM((heads, reqs, HD), jnp.bfloat16),
            pltpu.VMEM((blocks, merged, block), jnp.float32),
            pltpu.VMEM(out_proj.shape, jnp.bfloat16),
            pltpu.VMEM((groups, merged, heads // groups * HD), jnp.bfloat16),
            dma((10,)),
            dma((back // 2, groups, 2, CUTS)),
            dma((back // 2, groups, 2, CUTS)),
            dma((back // 2, groups, 2, CUTS)),
            dma((back // 2, groups, 2, CUTS)),
            dma((2,)),
            dma((n, 2)),
            dma((n // 2,)),
            dma((2,)),
            dma((groups,)),
            dma((groups,)),
            dma((groups,)),
            dma((groups,)),
            pltpu.SemaphoreType.REGULAR,
        ],
        compiler_params=pltpu.CompilerParams(
            collective_id=0, has_side_effects=True, vmem_limit_bytes=48 * 1024 * 1024
        ),
    )(*[pltpu.with_memory_space_constraint(x, pltpu.HBM) for x in args])
    return pl.pallas_call(
        put,
        out_shape=tuple(jax.ShapeDtypeStruct(x.shape, x.dtype) for x in result),
        in_specs=[vmem, vmem],
        out_specs=(hbm, hbm),
        scratch_shapes=[dma((2,))],
        compiler_params=pltpu.CompilerParams(vmem_limit_bytes=4 * 1024 * 1024),
    )(*result)


def solution(mesh):
    placed = (
        P(("rep", "seq"), "tp"),
        P(("rep", "seq"), "tp"),
        P(("rep", "seq"), "tp"),
        P("rep"),
        P("tp"),
        P("rep", "tp"),
        P("rep", "tp"),
        P("rep", "tp"),
        P(("rep", "seq"), "tp"),
        P(("rep", "seq"), "tp"),
        P(("rep", "seq")),
        P("rep"),
        P("tp", None),
    )
    return jax.shard_map(
        functools.partial(on_device, mesh.shape["seq"]),
        mesh=mesh,
        in_specs=placed,
        out_specs=(P(("rep", "seq", "tp"), None), P(("rep", "tp"), None)),
        check_vma=False,
    )
```

```python
import functools
import math

import jax
import jax.numpy as jnp
from jax import lax
from jax.experimental import pallas as pl
from jax.experimental.pallas import tpu as pltpu
from jax.sharding import PartitionSpec as P

HD = 128
WINDOW = 4096
PAGE = 128
DOCS = 4
MASKED = -1e30
FLOOR = -1e29
NEAR = WINDOW // 4
SUB = 256
CUTS = 2
MESH = pl.DeviceIdType.MESH


def dot_t(a, b):
    return lax.dot_general(a, b, (((1,), (1,)), ((), ())), preferred_element_type=jnp.float32)


def wide(column, width):
    return jnp.concatenate([column] * (width // column.shape[1]), axis=1)


def put(block_p, block_d, out_p, out_d, sem):
    copies = [
        pltpu.make_async_copy(block_p, out_p, sem.at[0]),
        pltpu.make_async_copy(block_d, out_d, sem.at[1]),
    ]
    for copy in copies:
        copy.start()
    for copy in copies:
        copy.wait()


def kernel(
    n, back, reach, pages_request, q_hbm, k_hbm, v_hbm, docs_hbm, windows, order, lengths,
    dq_hbm, dk_hbm, dv_hbm, ck, cv, w,
    out_p, out_d,
    q, k, v, docs, dq, dk, dv,
    kv, top, acc, lo, rows, ckv, cvv, wv, spread, pieces, part, stats, gathered, gathered_stats,
    att, total, wx, incoming,
    local_sem, zs, zr, ys, yr, ps, pr, fs, fr, ts, tr, ws, wr, gate,
):
    me = lax.axis_index("seq")
    core = lax.axis_index("tp")
    other = 1 - core
    odd = lax.rem(me, 2)
    partner = me + 1 - 2 * odd
    tokens = q.shape[0]
    heads = q.shape[1] // HD
    groups = k.shape[1] // HD
    per = heads // groups
    reqs = dq.shape[0]
    pages = order.shape[0]
    scale = 1.0 / math.sqrt(HD)
    exp_scale = scale * math.log2(math.e)

    pairs = (
        (k_hbm, k), (v_hbm, v), (dq_hbm, dq), (ck, ckv), (cv, cvv), (docs_hbm, docs), (q_hbm, q),
        (dk_hbm, dk), (dv_hbm, dv), (w, wv),
    )
    loads = [pltpu.make_async_copy(a, b, local_sem.at[i]) for i, (a, b) in enumerate(pairs)]
    for load in loads[:7]:
        load.start()

    barrier = pltpu.get_barrier_semaphore()

    @pl.when(me >= 2)
    def _():
        pl.semaphore_signal(barrier, inc=1, device_id={"seq": me - 2}, device_id_type=MESH)

    pl.semaphore_signal(barrier, inc=1, device_id={"seq": partner}, device_id_type=MESH)
    pl.semaphore_signal(barrier, inc=1, device_id={"tp": other}, device_id_type=MESH)
    pl.semaphore_wait(barrier, 2 + (me + 2 < n).astype(jnp.int32))

    def pass_gate():
        @pl.when(me >= 2)
        def _():
            pl.semaphore_wait(gate, 1)

        @pl.when(me + 2 < n)
        def _():
            pl.semaphore_signal(gate, inc=1, device_id={"seq": me + 2}, device_id_type=MESH)

    piece = tokens // CUTS

    def source(s, g, i, c):
        span = pl.ds(c * piece, piece)
        if s == 0:
            return (k, v)[i].at[span, pl.ds(g * HD, HD)]
        return kv.at[s - 1, g, i, span]

    def along(s, g, i, c):
        return pltpu.make_async_remote_copy(
            src_ref=source(s, g, i, c),
            dst_ref=kv.at[s + 1, g, i, pl.ds(c * piece, piece)],
            send_sem=zs.at[s // 2, g, i, c],
            recv_sem=zr.at[s // 2, g, i, c],
            device_id={"seq": lax.rem(me + 2, n)},
            device_id_type=MESH,
        )

    def across(s, h, g, i, c):
        return pltpu.make_async_remote_copy(
            src_ref=source(s, g, i, c),
            dst_ref=kv.at[2 * h - 2, g, i, pl.ds(c * piece, piece)],
            send_sem=ys.at[h - 1, g, i, c],
            recv_sem=yr.at[h - 1, g, i, c],
            device_id={"seq": partner},
            device_id_type=MESH,
        )

    def forward(s, g, finish=False, only=tuple((i, c) for c in range(CUTS) for i in range(2))):
        act = (lambda c: c.wait_send()) if finish else (lambda c: c.start())
        if s + 2 <= back:
            @pl.when((me >= s) & (me + 2 < n))
            def _():
                for i, c in only:
                    act(along(s, g, i, c))

            @pl.when((me >= s) & (odd == 0))
            def _():
                for i, c in only:
                    act(across(s, s // 2 + 1, g, i, c))
        if s >= 2:
            @pl.when((me >= s) & (odd == 1))
            def _():
                for i, c in only:
                    act(across(s, s // 2, g, i, c))

    order_of = tuple((i, c) for c in range(CUTS) for i in range(2))

    def arrive(s, g, only=order_of):
        for i, c in only:
            @pl.when(me >= s)
            def _():
                if s % 2 == 0:
                    along(s - 2, g, i, c).wait_recv()
                else:
                    across(s + 1, (s + 1) // 2, g, i, c).wait_recv()

            if s % 2 == 0:
                forward(s, g, only=((i, c),))

    def attend(s, g, low=0, top_key=None):
        def one_head(head):
            lanes = slice(g * HD, (g + 1) * HD)
            size = math.gcd(tokens, SUB)
            for r in range(0, tokens, size):
                cut = slice(r, r + size)
                first = max(low, (s * tokens + r - reach + 1) // HD * HD)
                last = min(r + size if s == 0 else tokens, top_key or tokens)
                if first >= last:
                    continue
                span = last - first
                queries = q[cut, head * HD:(head + 1) * HD]
                part_of = slice(first, last)
                keys = k[part_of, lanes] if s == 0 else kv[s - 1, g, 0, part_of]
                values = v[part_of, lanes] if s == 0 else kv[s - 1, g, 1, part_of]
                values = jnp.concatenate([values, jnp.ones_like(values)], axis=1)
                scores = dot_t(queries, keys)
                limit = lo[cut]
                if (s + 1) * tokens > NEAR:
                    place = me * tokens + r + lax.broadcasted_iota(jnp.int32, (size, HD), 0)
                    limit = jnp.maximum(limit, place - windows[head] + 1)
                limit = limit - ((me - s) * tokens + first)
                column = lax.broadcasted_iota(jnp.int32, (size, span), 1)
                allowed = column >= wide(limit, span)
                if s == 0:
                    allowed = allowed & (
                        column <= lax.broadcasted_iota(jnp.int32, (size, span), 0) + r
                    )
                scores = jnp.where(allowed, scores, MASKED)
                high = jnp.max(scores, axis=1, keepdims=True) * exp_scale
                high = jnp.broadcast_to(high, (size, HD))
                if s > 0:
                    old = top[head, cut]
                    high = jnp.maximum(high, old)
                weights = jnp.exp2(scores * exp_scale - wide(high, span))
                added = jnp.dot(
                    weights.astype(jnp.bfloat16), values,
                    preferred_element_type=jnp.float32,
                )
                if s > 0:
                    added = added + acc[head, cut] * wide(jnp.exp2(old - high), 2 * HD)
                top[head, cut] = high
                acc[head, cut] = added

        @pl.when(me >= s)
        def _():
            for r in range(per):
                one_head(g * per + r)

    def to_owner(j, g):
        span = pl.ds(g * per, per)
        sends = [(part.at[span], gathered.at[j, span])]
        if g == 0:
            sends.insert(0, (stats, gathered_stats.at[j]))
        return [
            pltpu.make_async_remote_copy(
                src_ref=src,
                dst_ref=dst,
                send_sem=ps.at[g + i * groups],
                recv_sem=pr.at[j, g + i * groups],
                device_id={"seq": 0},
                device_id_type=MESH,
            )
            for i, (src, dst) in enumerate(reversed(sends))
        ]

    def decode_partials():
        for i in (2, 3, 4):
            loads[i].wait()
        spread[...] = jnp.zeros_like(spread)
        for head in range(heads):
            g = head // per
            spread[:, head, g * HD:(g + 1) * HD] = (
                dq[:, head * HD:(head + 1) * HD].astype(jnp.float32)
            )
        step = math.gcd(pages, 8)
        lane = lax.broadcasted_iota(jnp.int32, (heads, PAGE), 1)
        group = lax.broadcasted_iota(jnp.int32, (heads, HD), 0) // per

        def block(b, carry):
            levels, owners = carry
            scores, spans, who = [], [], []
            for i in range(step):
                page = order[b * step + i]
                owner = page // pages_request
                left = lengths[owner] - (page - owner * pages_request) * PAGE
                span = pl.ds(pl.multiple_of((b * step + i) * PAGE, PAGE), PAGE)
                score = dot_t(spread[owner].astype(jnp.bfloat16), ckv[span, :])
                scores.append(jnp.where(lane < left, score, MASKED))
                spans.append(span)
                who.append(owner)
            scores = jnp.concatenate(scores, axis=0)
            high = jnp.max(scores, axis=1, keepdims=True)
            high = jnp.broadcast_to(jnp.maximum(high, FLOOR) * exp_scale, scores.shape)
            weights = jnp.exp2(scores * exp_scale - high)
            total = jnp.broadcast_to(jnp.sum(weights, axis=1, keepdims=True), scores.shape)
            some = total > 0.0
            whole = jnp.where(some, total, 1.0)
            level = jnp.where(some, high + jnp.log2(whole), FLOOR)
            weights = (weights / whole).astype(jnp.bfloat16)
            for i in range(step):
                cut = slice(i * heads, (i + 1) * heads)
                both = jnp.dot(
                    weights[cut], cvv[spans[i], :], preferred_element_type=jnp.float32
                )
                mixed = both[:, :HD]
                for g in range(1, groups):
                    mixed = jnp.where(group == g, both[:, g * HD:(g + 1) * HD], mixed)
                pieces[b * step + i] = mixed
                here = lane == b * step + i
                levels = jnp.where(here, level[cut], levels)
                owners = jnp.where(here, who[i].astype(jnp.float32), owners)
            return (levels, owners)

        blank = jnp.zeros((heads, PAGE), jnp.float32)
        levels, owners = lax.fori_loop(
            0, pages // step, block, (blank + FLOOR, blank - 1.0)
        )
        stats[:heads] = levels
        stats[heads:] = owners
        for head in range(heads):
            part[head] = pieces[:, head].astype(jnp.bfloat16)

        @pl.when(me > 0)
        def _():
            for g in range(groups):
                for copy in to_owner(me, g):
                    copy.start()

    levels = n // 2
    near = max(levels // 2, 1)

    def finals(level, g):
        span = pl.ds(g * per, per)
        return pltpu.make_async_remote_copy(
            src_ref=att.at[span],
            dst_ref=att.at[span],
            send_sem=fs.at[level, g],
            recv_sem=fr.at[0 if level else 1, g],
            device_id={"seq": 2 * level if level else partner},
            device_id_type=MESH,
        )

    def publish(g, finish=False):
        for level in range(min(near, levels - 1), -1, -1):
            if finish:
                finals(level, g).wait_send()
            else:
                finals(level, g).start()

    relays = range(2, levels - near + 1)

    def relay(g):
        for level in range(near + 1, levels):
            @pl.when(me == 2 * (level - near + 1))
            def _():
                finals(1, g).wait_recv()
                finals(level, g).start()

    def share(g):
        waiting = (odd == 0) & (me >= 2)
        for level in relays:
            waiting = waiting & (me != 2 * level)

        @pl.when(waiting)
        def _():
            finals(1, g).wait_recv()

        @pl.when((odd == 0) & (me >= 2))
        def _():
            finals(0, g).start()

    def decode_merge():
        @pl.when(me == 0)
        def _():
            loads[7].wait()
            loads[8].wait()
            gathered[0] = part[...]
            gathered_stats[0] = stats[...]
            request = lax.broadcasted_iota(jnp.int32, (reqs, PAGE), 0).astype(jnp.float32)

            def one_head(r):
                queries = dq[:, r * HD:(r + 1) * HD].astype(jnp.float32)
                group = slice(r // per * HD, (r // per + 1) * HD)
                own = jnp.sum(queries * dk[:, group].astype(jnp.float32), axis=1, keepdims=True)
                own = jnp.broadcast_to(own * exp_scale, (reqs, HD))
                levels = [
                    jnp.where(
                        gathered_stats[j, heads:heads + 1, :] == request,
                        gathered_stats[j, r:r + 1, :], FLOOR,
                    )
                    for j in range(n)
                ]
                high = functools.reduce(jnp.maximum, levels)
                high = jnp.broadcast_to(jnp.max(high, axis=1, keepdims=True), own.shape)
                high = jnp.maximum(own, high)
                mine = jnp.exp2(own - high)
                weights = [jnp.exp2(level - high) for level in levels]
                count = jnp.sum(sum(weights), axis=1, keepdims=True)
                summed = mine * dv[:, group].astype(jnp.float32)
                for j in range(n):
                    summed = summed + jnp.dot(
                        weights[j][:, :pages].astype(jnp.bfloat16), gathered[j, r],
                        preferred_element_type=jnp.float32,
                    )
                att[r] = (summed / (mine + count)).astype(jnp.bfloat16)

            for g in range(groups):
                for j in range(1, n):
                    for copy in to_owner(j, g):
                        copy.wait_recv()
                for r in range(g * per, (g + 1) * per):
                    one_head(r)
                publish(g)

    half = tokens // 2
    half_reqs = reqs // 2
    wide_rows = per * HD
    width = total.shape[2]
    blocks = total.shape[0]

    def borrow(g):
        span = pl.ds(g * wide_rows, wide_rows)
        return pltpu.make_async_remote_copy(
            src_ref=w.at[span],
            dst_ref=wx.at[span],
            send_sem=ws.at[g],
            recv_sem=wr.at[g],
            device_id={"tp": other},
            device_id_type=MESH,
        )

    def exchange(g):
        return pltpu.make_async_remote_copy(
            src_ref=rows.at[g, other],
            dst_ref=incoming.at[g],
            send_sem=ts.at[g],
            recv_sem=tr.at[g],
            device_id={"tp": other},
            device_id_type=MESH,
        )

    def settle(g):
        for r in range(per):
            head = g * per + r
            cut = slice(r * HD, (r + 1) * HD)
            done = (acc[head, :, :HD] / acc[head, :, HD:]).astype(jnp.bfloat16)
            for c in range(2):
                rows[g, c, :half, cut] = done[c * half:(c + 1) * half]
                rows[g, c, half:, cut] = att[head, c * half_reqs:(c + 1) * half_reqs]
        exchange(g).start()

    def project(g, mine):
        weights = wv if mine else wx
        depth = slice(g * wide_rows, (g + 1) * wide_rows)
        first = mine and g == 0
        last = not mine and g == groups - 1

        def block(b, carry):
            span = pl.ds(pl.multiple_of(b * width, width), width)
            left = rows[g, core] if mine else incoming[g]
            added = jnp.dot(left, weights[depth, span], preferred_element_type=jnp.float32)
            if not first:
                added = added + total[b]
            if last:
                out_p[:, span] = added[:half].astype(jnp.bfloat16)
                out_d[:, span] = added[half:].astype(jnp.bfloat16)
            else:
                total[b] = added
            return carry

        lax.fori_loop(0, blocks, block, 0)

    for i in (0, 1):
        loads[i].wait()
    for g in range(groups):
        forward(0, g)
    pass_gate()
    decode_partials()
    for load in loads[7:]:
        load.start()
    for g in range(groups):
        borrow(g).start()
    loads[5].wait()
    position = me * tokens + lax.broadcasted_iota(jnp.int32, (tokens, HD), 0)
    place = position.astype(jnp.float32)
    start = jnp.zeros((tokens, HD), jnp.float32)
    for document in range(1, DOCS):
        before = (docs[...] < document).astype(jnp.float32)
        before = jnp.sum(jnp.sum(before, axis=0, keepdims=True), axis=1, keepdims=True)
        start = jnp.where(before <= place, jnp.maximum(start, before), start)
    lo[...] = start.astype(jnp.int32)
    loads[6].wait()
    steps = [(s, g) for s in range(2, back + 1, 2) for g in range(groups)]
    arrive(*steps[0], order_of[:1])
    for g in range(groups):
        attend(0, g)
        if g == 0:
            arrive(*steps[0], order_of[1:2])
    decode_merge()

    def obtain(g):
        @pl.when(odd == 1)
        def _():
            finals(0, g).wait_recv()

    def early():
        obtain(0)
        settle(0)
        loads[9].wait()
        project(0, True)

    def middle():
        for i in range(groups):
            borrow(i).wait_recv()
        exchange(0).wait_recv()
        if groups > 1:
            project(0, False)

    for step, (s, g) in enumerate(steps):
        later = steps[step + 1:step + 2]
        arrive(s, g, order_of[2:])
        attend(s, g)
        for following in later:
            arrive(*following, order_of[:1])
        if not later:
            for i in range(1, groups):
                share(i)

            @pl.when(odd == 0)
            def _():
                if step == 0 or groups == 1:
                    early()
                middle()

            arrive(s - 1, g)
            attend(s - 1, g)

            @pl.when(odd == 1)
            def _():
                early()
                middle()

        else:
            if s == back and g == 0:
                for i in range(1, groups):
                    relay(i)
            arrive(s - 1, g)
            attend(s - 1, g)
        for following in later:
            arrive(*following, order_of[1:2])
        if s == 2 and g == groups - 1:
            relay(0)
        if s == back and g == 0:
            share(0)
            if groups > 1:
                pl.when(odd == 0)(early)
    for g in range(1, groups):
        obtain(g)
        settle(g)
        project(g, True)
        exchange(g).wait_recv()
        if g < groups - 1:
            project(g, False)
    project(groups - 1, False)

    for g in range(groups):
        exchange(g).wait_send()
        borrow(g).wait_send()
    for s in range(0, back + 1, 2):
        for g in range(groups):
            forward(s, g, finish=True)
    @pl.when(me > 0)
    def _():
        for g in range(groups):
            for copy in to_owner(me, g):
                copy.wait_send()
        loads[7].wait()
        loads[8].wait()

    for g in range(groups):
        @pl.when(me == 0)
        def _():
            publish(g, True)

        for level in range(near + 1, levels):
            @pl.when(me == 2 * (level - near + 1))
            def _():
                finals(level, g).wait_send()

        @pl.when((odd == 0) & (me >= 2))
        def _():
            finals(0, g).wait_send()


def on_device(
    n, prefill_query, prefill_key, prefill_value, doc_ids, head_window, dec_query, dec_key,
    dec_value, cache_key, cache_value, page_order, lengths, out_proj,
):
    tokens, width = prefill_query.shape
    heads = width // HD
    groups = prefill_key.shape[1] // HD
    reqs = dec_query.shape[0]
    model = out_proj.shape[1]
    pages = page_order.shape[0]
    reach = min(doc_ids.shape[0] // 2, WINDOW)
    back = -(-reach // tokens)
    back += back % 2

    pages_request = page_order.shape[0] * n // reqs
    docs = doc_ids.reshape(-1, HD)
    vmem = pl.BlockSpec(memory_space=pltpu.VMEM)
    hbm = pl.BlockSpec(memory_space=pltpu.HBM)
    smem = pl.BlockSpec(memory_space=pltpu.SMEM)
    block = 4096
    blocks = model // block
    merged = (tokens + reqs) // 2
    dma = pltpu.SemaphoreType.DMA
    args = (
        prefill_query, prefill_key, prefill_value, docs, head_window, page_order, lengths,
        dec_query, dec_key, dec_value, cache_key, cache_value, out_proj,
    )
    result = pl.pallas_call(
        functools.partial(kernel, n, back, reach, pages_request),
        out_shape=(
            jax.ShapeDtypeStruct((tokens // 2, model), jnp.bfloat16),
            jax.ShapeDtypeStruct((reqs // 2, model), jnp.bfloat16),
        ),
        in_specs=[hbm] * 4 + [smem] * 3 + [hbm] * 6,
        out_specs=(vmem, vmem),
        scratch_shapes=[
            pltpu.VMEM(prefill_query.shape, jnp.bfloat16),
            pltpu.VMEM(prefill_key.shape, jnp.bfloat16),
            pltpu.VMEM(prefill_value.shape, jnp.bfloat16),
            pltpu.VMEM(docs.shape, jnp.int32),
            pltpu.VMEM(dec_query.shape, jnp.bfloat16),
            pltpu.VMEM(dec_key.shape, jnp.bfloat16),
            pltpu.VMEM(dec_value.shape, jnp.bfloat16),
            pltpu.VMEM((back, groups, 2, tokens, HD), jnp.bfloat16),
            pltpu.VMEM((heads, tokens, HD), jnp.float32),
            pltpu.VMEM((heads, tokens, 2 * HD), jnp.float32),
            pltpu.VMEM((tokens, HD), jnp.int32),
            pltpu.VMEM((groups, 2, merged, heads // groups * HD), jnp.bfloat16),
            pltpu.VMEM(cache_key.shape, jnp.bfloat16),
            pltpu.VMEM(cache_value.shape, jnp.bfloat16),
            pltpu.VMEM(out_proj.shape, jnp.bfloat16),
            pltpu.VMEM((reqs, heads, groups * HD), jnp.float32),
            pltpu.VMEM((pages, heads, HD), jnp.float32),
            pltpu.VMEM((heads, pages, HD), jnp.bfloat16),
            pltpu.VMEM((2 * heads, PAGE), jnp.float32),
            pltpu.VMEM((n, heads, pages, HD), jnp.bfloat16),
            pltpu.VMEM((n, 2 * heads, PAGE), jnp.float32),
            pltpu.VMEM((heads, reqs, HD), jnp.bfloat16),
            pltpu.VMEM((blocks, merged, block), jnp.float32),
            pltpu.VMEM(out_proj.shape, jnp.bfloat16),
            pltpu.VMEM((groups, merged, heads // groups * HD), jnp.bfloat16),
            dma((10,)),
            dma((back // 2, groups, 2, CUTS)),
            dma((back // 2, groups, 2, CUTS)),
            dma((back // 2, groups, 2, CUTS)),
            dma((back // 2, groups, 2, CUTS)),
            dma((groups + 1,)),
            dma((n, groups + 1)),
            dma((n // 2, groups)),
            dma((2, groups)),
            dma((groups,)),
            dma((groups,)),
            dma((groups,)),
            dma((groups,)),
            pltpu.SemaphoreType.REGULAR,
        ],
        compiler_params=pltpu.CompilerParams(
            collective_id=0, has_side_effects=True, vmem_limit_bytes=48 * 1024 * 1024
        ),
    )(*[pltpu.with_memory_space_constraint(x, pltpu.HBM) for x in args])
    return pl.pallas_call(
        put,
        out_shape=tuple(jax.ShapeDtypeStruct(x.shape, x.dtype) for x in result),
        in_specs=[vmem, vmem],
        out_specs=(hbm, hbm),
        scratch_shapes=[dma((2,))],
        compiler_params=pltpu.CompilerParams(vmem_limit_bytes=4 * 1024 * 1024),
    )(*result)


def solution(mesh):
    placed = (
        P(("rep", "seq"), "tp"),
        P(("rep", "seq"), "tp"),
        P(("rep", "seq"), "tp"),
        P("rep"),
        P("tp"),
        P("rep", "tp"),
        P("rep", "tp"),
        P("rep", "tp"),
        P(("rep", "seq"), "tp"),
        P(("rep", "seq"), "tp"),
        P(("rep", "seq")),
        P("rep"),
        P("tp", None),
    )
    return jax.shard_map(
        functools.partial(on_device, mesh.shape["seq"]),
        mesh=mesh,
        in_specs=placed,
        out_specs=(P(("rep", "seq", "tp"), None), P(("rep", "tp"), None)),
        check_vma=False,
    )
```

```python
import functools
import math

import jax
import jax.numpy as jnp
from jax import lax
from jax.experimental import pallas as pl
from jax.experimental.pallas import tpu as pltpu
from jax.sharding import PartitionSpec as P

HD = 128
WINDOW = 4096
PAGE = 128
DOCS = 4
MASKED = -1e30
FLOOR = -1e29
NEAR = WINDOW // 4
SUB = 256
CUTS = 2
MESH = pl.DeviceIdType.MESH


def dot_t(a, b):
    return lax.dot_general(a, b, (((1,), (1,)), ((), ())), preferred_element_type=jnp.float32)


def wide(column, width):
    return jnp.concatenate([column] * (width // column.shape[1]), axis=1)


def put(block_p, block_d, out_p, out_d, sem):
    copies = [
        pltpu.make_async_copy(block_p, out_p, sem.at[0]),
        pltpu.make_async_copy(block_d, out_d, sem.at[1]),
    ]
    for copy in copies:
        copy.start()
    for copy in copies:
        copy.wait()


def kernel(
    n, back, reach, pages_request, q_hbm, k_hbm, v_hbm, docs_hbm, windows, order, lengths,
    dq_hbm, dk_hbm, dv_hbm, ck, cv, w,
    out_p, out_d,
    q, k, v, docs, dq, dk, dv,
    kv, top, acc, lo, rows, ckv, cvv, wv, spread, pieces, part, stats, gathered, gathered_stats,
    att, total, wx, incoming,
    local_sem, zs, zr, ys, yr, ps, pr, fs, fr, ts, tr, ws, wr, gate,
):
    me = lax.axis_index("seq")
    core = lax.axis_index("tp")
    other = 1 - core
    odd = lax.rem(me, 2)
    partner = me + 1 - 2 * odd
    tokens = q.shape[0]
    heads = q.shape[1] // HD
    groups = k.shape[1] // HD
    per = heads // groups
    reqs = dq.shape[0]
    pages = order.shape[0]
    scale = 1.0 / math.sqrt(HD)
    exp_scale = scale * math.log2(math.e)

    pairs = (
        (k_hbm, k), (v_hbm, v), (dq_hbm, dq), (ck, ckv), (cv, cvv), (docs_hbm, docs), (q_hbm, q),
        (dk_hbm, dk), (dv_hbm, dv), (w, wv),
    )
    loads = [pltpu.make_async_copy(a, b, local_sem.at[i]) for i, (a, b) in enumerate(pairs)]
    for i in (0, 1, 2, 5, 6):
        loads[i].start()

    barrier = pltpu.get_barrier_semaphore()

    @pl.when(me >= 2)
    def _():
        pl.semaphore_signal(barrier, inc=1, device_id={"seq": me - 2}, device_id_type=MESH)

    pl.semaphore_signal(barrier, inc=1, device_id={"seq": partner}, device_id_type=MESH)
    pl.semaphore_signal(barrier, inc=1, device_id={"tp": other}, device_id_type=MESH)
    pl.semaphore_wait(barrier, 2 + (me + 2 < n).astype(jnp.int32))

    def pass_gate():
        @pl.when(me >= 2)
        def _():
            pl.semaphore_wait(gate, 1)

        @pl.when(me + 2 < n)
        def _():
            pl.semaphore_signal(gate, inc=1, device_id={"seq": me + 2}, device_id_type=MESH)

    piece = tokens // CUTS

    def source(s, g, i, c):
        span = pl.ds(c * piece, piece)
        if s == 0:
            return (k, v)[i].at[span, pl.ds(g * HD, HD)]
        return kv.at[s - 1, g, i, span]

    def along(s, g, i, c):
        return pltpu.make_async_remote_copy(
            src_ref=source(s, g, i, c),
            dst_ref=kv.at[s + 1, g, i, pl.ds(c * piece, piece)],
            send_sem=zs.at[s // 2, g, i, c],
            recv_sem=zr.at[s // 2, g, i, c],
            device_id={"seq": lax.rem(me + 2, n)},
            device_id_type=MESH,
        )

    def across(s, h, g, i, c):
        return pltpu.make_async_remote_copy(
            src_ref=source(s, g, i, c),
            dst_ref=kv.at[2 * h - 2, g, i, pl.ds(c * piece, piece)],
            send_sem=ys.at[h - 1, g, i, c],
            recv_sem=yr.at[h - 1, g, i, c],
            device_id={"seq": partner},
            device_id_type=MESH,
        )

    def forward(s, g, finish=False, only=tuple((i, c) for c in range(CUTS) for i in range(2))):
        act = (lambda c: c.wait_send()) if finish else (lambda c: c.start())
        if s + 2 <= back:
            @pl.when((me >= s) & (me + 2 < n))
            def _():
                for i, c in only:
                    act(along(s, g, i, c))

            @pl.when((me >= s) & (odd == 0))
            def _():
                for i, c in only:
                    act(across(s, s // 2 + 1, g, i, c))
        if s >= 2:
            @pl.when((me >= s) & (odd == 1))
            def _():
                for i, c in only:
                    act(across(s, s // 2, g, i, c))

    order_of = tuple((i, c) for c in range(CUTS) for i in range(2))

    def arrive(s, g, only=order_of):
        for i, c in only:
            @pl.when(me >= s)
            def _():
                if s % 2 == 0:
                    along(s - 2, g, i, c).wait_recv()
                else:
                    across(s + 1, (s + 1) // 2, g, i, c).wait_recv()

            if s % 2 == 0:
                forward(s, g, only=((i, c),))

    def attend(s, g, low=0, top_key=None):
        def one_head(head):
            lanes = slice(g * HD, (g + 1) * HD)
            size = math.gcd(tokens, SUB)
            for r in range(0, tokens, size):
                cut = slice(r, r + size)
                first = max(low, (s * tokens + r - reach + 1) // HD * HD)
                last = min(r + size if s == 0 else tokens, top_key or tokens)
                if first >= last:
                    continue
                span = last - first
                queries = q[cut, head * HD:(head + 1) * HD]
                part_of = slice(first, last)
                keys = k[part_of, lanes] if s == 0 else kv[s - 1, g, 0, part_of]
                values = v[part_of, lanes] if s == 0 else kv[s - 1, g, 1, part_of]
                values = jnp.concatenate([values, jnp.ones_like(values)], axis=1)
                scores = dot_t(queries, keys)
                limit = lo[cut]
                if (s + 1) * tokens > NEAR:
                    place = me * tokens + r + lax.broadcasted_iota(jnp.int32, (size, HD), 0)
                    limit = jnp.maximum(limit, place - windows[head] + 1)
                limit = limit - ((me - s) * tokens + first)
                column = lax.broadcasted_iota(jnp.int32, (size, span), 1)
                allowed = column >= wide(limit, span)
                if s == 0:
                    allowed = allowed & (
                        column <= lax.broadcasted_iota(jnp.int32, (size, span), 0) + r
                    )
                scores = jnp.where(allowed, scores, MASKED)
                high = jnp.max(scores, axis=1, keepdims=True) * exp_scale
                high = jnp.broadcast_to(high, (size, HD))
                if s > 0:
                    old = top[head, cut]
                    high = jnp.maximum(high, old)
                weights = jnp.exp2(scores * exp_scale - wide(high, span))
                added = jnp.dot(
                    weights.astype(jnp.bfloat16), values,
                    preferred_element_type=jnp.float32,
                )
                if s > 0:
                    added = added + acc[head, cut] * wide(jnp.exp2(old - high), 2 * HD)
                top[head, cut] = high
                acc[head, cut] = added

        @pl.when(me >= s)
        def _():
            for r in range(per):
                one_head(g * per + r)

    def to_owner(j, g):
        span = pl.ds(g * per, per)
        sends = [(part.at[span], gathered.at[j, span])]
        if g == 0:
            sends.insert(0, (stats, gathered_stats.at[j]))
        return [
            pltpu.make_async_remote_copy(
                src_ref=src,
                dst_ref=dst,
                send_sem=ps.at[g + i * groups],
                recv_sem=pr.at[j, g + i * groups],
                device_id={"seq": 0},
                device_id_type=MESH,
            )
            for i, (src, dst) in enumerate(reversed(sends))
        ]

    def decode_partials():
        for i in (2, 3, 4):
            loads[i].wait()
        spread[...] = jnp.zeros_like(spread)
        for head in range(heads):
            g = head // per
            spread[:, head, g * HD:(g + 1) * HD] = (
                dq[:, head * HD:(head + 1) * HD].astype(jnp.float32)
            )
        step = math.gcd(pages, 8)
        lane = lax.broadcasted_iota(jnp.int32, (heads, PAGE), 1)
        group = lax.broadcasted_iota(jnp.int32, (heads, HD), 0) // per

        def block(b, carry):
            levels, owners = carry
            scores, spans, who = [], [], []
            for i in range(step):
                page = order[b * step + i]
                owner = page // pages_request
                left = lengths[owner] - (page - owner * pages_request) * PAGE
                span = pl.ds(pl.multiple_of((b * step + i) * PAGE, PAGE), PAGE)
                score = dot_t(spread[owner].astype(jnp.bfloat16), ckv[span, :])
                scores.append(jnp.where(lane < left, score, MASKED))
                spans.append(span)
                who.append(owner)
            scores = jnp.concatenate(scores, axis=0)
            high = jnp.max(scores, axis=1, keepdims=True)
            high = jnp.broadcast_to(jnp.maximum(high, FLOOR) * exp_scale, scores.shape)
            weights = jnp.exp2(scores * exp_scale - high)
            total = jnp.broadcast_to(jnp.sum(weights, axis=1, keepdims=True), scores.shape)
            some = total > 0.0
            whole = jnp.where(some, total, 1.0)
            level = jnp.where(some, high + jnp.log2(whole), FLOOR)
            weights = (weights / whole).astype(jnp.bfloat16)
            for i in range(step):
                cut = slice(i * heads, (i + 1) * heads)
                both = jnp.dot(
                    weights[cut], cvv[spans[i], :], preferred_element_type=jnp.float32
                )
                mixed = both[:, :HD]
                for g in range(1, groups):
                    mixed = jnp.where(group == g, both[:, g * HD:(g + 1) * HD], mixed)
                pieces[b * step + i] = mixed
                here = lane == b * step + i
                levels = jnp.where(here, level[cut], levels)
                owners = jnp.where(here, who[i].astype(jnp.float32), owners)
            return (levels, owners)

        blank = jnp.zeros((heads, PAGE), jnp.float32)
        levels, owners = lax.fori_loop(
            0, pages // step, block, (blank + FLOOR, blank - 1.0)
        )
        stats[:heads] = levels
        stats[heads:] = owners
        for head in range(heads):
            part[head] = pieces[:, head].astype(jnp.bfloat16)

        @pl.when(me > 0)
        def _():
            for g in range(groups):
                for copy in to_owner(me, g):
                    copy.start()

    levels = n // 2
    near = max(levels // 2, 1)

    def finals(level, g):
        span = pl.ds(g * per, per)
        return pltpu.make_async_remote_copy(
            src_ref=att.at[span],
            dst_ref=att.at[span],
            send_sem=fs.at[level, g],
            recv_sem=fr.at[0 if level else 1, g],
            device_id={"seq": 2 * level if level else partner},
            device_id_type=MESH,
        )

    def publish(g, finish=False):
        for level in range(min(near, levels - 1), -1, -1):
            if finish:
                finals(level, g).wait_send()
            else:
                finals(level, g).start()

    relays = range(2, levels - near + 1)

    def relay(g):
        for level in range(near + 1, levels):
            @pl.when(me == 2 * (level - near + 1))
            def _():
                finals(1, g).wait_recv()
                finals(level, g).start()

    def share(g):
        waiting = (odd == 0) & (me >= 2)
        for level in relays:
            waiting = waiting & (me != 2 * level)

        @pl.when(waiting)
        def _():
            finals(1, g).wait_recv()

        @pl.when((odd == 0) & (me >= 2))
        def _():
            finals(0, g).start()

    def decode_merge():
        @pl.when(me == 0)
        def _():
            loads[7].wait()
            loads[8].wait()
            gathered[0] = part[...]
            gathered_stats[0] = stats[...]
            request = lax.broadcasted_iota(jnp.int32, (reqs, PAGE), 0).astype(jnp.float32)

            def one_head(r):
                queries = dq[:, r * HD:(r + 1) * HD].astype(jnp.float32)
                group = slice(r // per * HD, (r // per + 1) * HD)
                own = jnp.sum(queries * dk[:, group].astype(jnp.float32), axis=1, keepdims=True)
                own = jnp.broadcast_to(own * exp_scale, (reqs, HD))
                levels = [
                    jnp.where(
                        gathered_stats[j, heads:heads + 1, :] == request,
                        gathered_stats[j, r:r + 1, :], FLOOR,
                    )
                    for j in range(n)
                ]
                high = functools.reduce(jnp.maximum, levels)
                high = jnp.broadcast_to(jnp.max(high, axis=1, keepdims=True), own.shape)
                high = jnp.maximum(own, high)
                mine = jnp.exp2(own - high)
                weights = [jnp.exp2(level - high) for level in levels]
                count = jnp.sum(sum(weights), axis=1, keepdims=True)
                summed = mine * dv[:, group].astype(jnp.float32)
                for j in range(n):
                    summed = summed + jnp.dot(
                        weights[j][:, :pages].astype(jnp.bfloat16), gathered[j, r],
                        preferred_element_type=jnp.float32,
                    )
                att[r] = (summed / (mine + count)).astype(jnp.bfloat16)

            for g in range(groups):
                for j in range(1, n):
                    for copy in to_owner(j, g):
                        copy.wait_recv()
                for r in range(g * per, (g + 1) * per):
                    one_head(r)
                publish(g)

    half = tokens // 2
    half_reqs = reqs // 2
    wide_rows = per * HD
    width = total.shape[2]
    blocks = total.shape[0]

    def borrow(g):
        span = pl.ds(g * wide_rows, wide_rows)
        return pltpu.make_async_remote_copy(
            src_ref=w.at[span],
            dst_ref=wx.at[span],
            send_sem=ws.at[g],
            recv_sem=wr.at[g],
            device_id={"tp": other},
            device_id_type=MESH,
        )

    def exchange(g):
        return pltpu.make_async_remote_copy(
            src_ref=rows.at[g, other],
            dst_ref=incoming.at[g],
            send_sem=ts.at[g],
            recv_sem=tr.at[g],
            device_id={"tp": other},
            device_id_type=MESH,
        )

    def settle(g):
        for r in range(per):
            head = g * per + r
            cut = slice(r * HD, (r + 1) * HD)
            done = (acc[head, :, :HD] / acc[head, :, HD:]).astype(jnp.bfloat16)
            for c in range(2):
                rows[g, c, :half, cut] = done[c * half:(c + 1) * half]
                rows[g, c, half:, cut] = att[head, c * half_reqs:(c + 1) * half_reqs]
        exchange(g).start()

    def project(g, mine):
        weights = wv if mine else wx
        depth = slice(g * wide_rows, (g + 1) * wide_rows)
        first = mine and g == 0
        last = not mine and g == groups - 1

        def block(b, carry):
            span = pl.ds(pl.multiple_of(b * width, width), width)
            left = rows[g, core] if mine else incoming[g]
            added = jnp.dot(left, weights[depth, span], preferred_element_type=jnp.float32)
            if not first:
                added = added + total[b]
            if last:
                out_p[:, span] = added[:half].astype(jnp.bfloat16)
                out_d[:, span] = added[half:].astype(jnp.bfloat16)
            else:
                total[b] = added
            return carry

        lax.fori_loop(0, blocks, block, 0)

    for i in (0, 1):
        loads[i].wait()
    for g in range(groups):
        forward(0, g)
    for i in (3, 4):
        loads[i].start()
    loads[5].wait()
    position = me * tokens + lax.broadcasted_iota(jnp.int32, (tokens, HD), 0)
    place = position.astype(jnp.float32)
    start = jnp.zeros((tokens, HD), jnp.float32)
    for document in range(1, DOCS):
        before = (docs[...] < document).astype(jnp.float32)
        before = jnp.sum(jnp.sum(before, axis=0, keepdims=True), axis=1, keepdims=True)
        start = jnp.where(before <= place, jnp.maximum(start, before), start)
    lo[...] = start.astype(jnp.int32)
    loads[6].wait()
    steps = [(s, g) for s in range(2, back + 1, 2) for g in range(groups)]
    for g in range(groups):
        attend(0, g)
        if g == 0:
            pass_gate()
            decode_partials()
            for load in loads[7:]:
                load.start()
            for g in range(groups):
                borrow(g).start()
            arrive(*steps[0], order_of[:2])
    decode_merge()

    def obtain(g):
        @pl.when(odd == 1)
        def _():
            finals(0, g).wait_recv()

    def early():
        obtain(0)
        settle(0)
        loads[9].wait()
        project(0, True)

    def middle():
        for i in range(groups):
            borrow(i).wait_recv()
        exchange(0).wait_recv()
        if groups > 1:
            project(0, False)

    for step, (s, g) in enumerate(steps):
        later = steps[step + 1:step + 2]
        arrive(s, g, order_of[2:])
        attend(s, g)
        for following in later:
            arrive(*following, order_of[:1])
        if not later:
            for i in range(1, groups):
                share(i)

            @pl.when(odd == 0)
            def _():
                if step == 0 or groups == 1:
                    early()
                middle()

            arrive(s - 1, g)
            attend(s - 1, g)

            @pl.when(odd == 1)
            def _():
                early()
                middle()

        else:
            if s == back and g == 0:
                for i in range(1, groups):
                    relay(i)
            arrive(s - 1, g)
            attend(s - 1, g)
        for following in later:
            arrive(*following, order_of[1:2])
        if s == 2 and g == groups - 1:
            relay(0)
        if s == back and g == 0:
            share(0)
            if groups > 1:
                pl.when(odd == 0)(early)
    for g in range(1, groups):
        obtain(g)
        settle(g)
        project(g, True)
        exchange(g).wait_recv()
        if g < groups - 1:
            project(g, False)
    project(groups - 1, False)

    for g in range(groups):
        exchange(g).wait_send()
        borrow(g).wait_send()
    for s in range(0, back + 1, 2):
        for g in range(groups):
            forward(s, g, finish=True)
    @pl.when(me > 0)
    def _():
        for g in range(groups):
            for copy in to_owner(me, g):
                copy.wait_send()
        loads[7].wait()
        loads[8].wait()

    for g in range(groups):
        @pl.when(me == 0)
        def _():
            publish(g, True)

        for level in range(near + 1, levels):
            @pl.when(me == 2 * (level - near + 1))
            def _():
                finals(level, g).wait_send()

        @pl.when((odd == 0) & (me >= 2))
        def _():
            finals(0, g).wait_send()


def on_device(
    n, prefill_query, prefill_key, prefill_value, doc_ids, head_window, dec_query, dec_key,
    dec_value, cache_key, cache_value, page_order, lengths, out_proj,
):
    tokens, width = prefill_query.shape
    heads = width // HD
    groups = prefill_key.shape[1] // HD
    reqs = dec_query.shape[0]
    model = out_proj.shape[1]
    pages = page_order.shape[0]
    reach = min(doc_ids.shape[0] // 2, WINDOW)
    back = -(-reach // tokens)
    back += back % 2

    pages_request = page_order.shape[0] * n // reqs
    docs = doc_ids.reshape(-1, HD)
    vmem = pl.BlockSpec(memory_space=pltpu.VMEM)
    hbm = pl.BlockSpec(memory_space=pltpu.HBM)
    smem = pl.BlockSpec(memory_space=pltpu.SMEM)
    block = 4096
    blocks = model // block
    merged = (tokens + reqs) // 2
    dma = pltpu.SemaphoreType.DMA
    args = (
        prefill_query, prefill_key, prefill_value, docs, head_window, page_order, lengths,
        dec_query, dec_key, dec_value, cache_key, cache_value, out_proj,
    )
    result = pl.pallas_call(
        functools.partial(kernel, n, back, reach, pages_request),
        out_shape=(
            jax.ShapeDtypeStruct((tokens // 2, model), jnp.bfloat16),
            jax.ShapeDtypeStruct((reqs // 2, model), jnp.bfloat16),
        ),
        in_specs=[hbm] * 4 + [smem] * 3 + [hbm] * 6,
        out_specs=(vmem, vmem),
        scratch_shapes=[
            pltpu.VMEM(prefill_query.shape, jnp.bfloat16),
            pltpu.VMEM(prefill_key.shape, jnp.bfloat16),
            pltpu.VMEM(prefill_value.shape, jnp.bfloat16),
            pltpu.VMEM(docs.shape, jnp.int32),
            pltpu.VMEM(dec_query.shape, jnp.bfloat16),
            pltpu.VMEM(dec_key.shape, jnp.bfloat16),
            pltpu.VMEM(dec_value.shape, jnp.bfloat16),
            pltpu.VMEM((back, groups, 2, tokens, HD), jnp.bfloat16),
            pltpu.VMEM((heads, tokens, HD), jnp.float32),
            pltpu.VMEM((heads, tokens, 2 * HD), jnp.float32),
            pltpu.VMEM((tokens, HD), jnp.int32),
            pltpu.VMEM((groups, 2, merged, heads // groups * HD), jnp.bfloat16),
            pltpu.VMEM(cache_key.shape, jnp.bfloat16),
            pltpu.VMEM(cache_value.shape, jnp.bfloat16),
            pltpu.VMEM(out_proj.shape, jnp.bfloat16),
            pltpu.VMEM((reqs, heads, groups * HD), jnp.float32),
            pltpu.VMEM((pages, heads, HD), jnp.float32),
            pltpu.VMEM((heads, pages, HD), jnp.bfloat16),
            pltpu.VMEM((2 * heads, PAGE), jnp.float32),
            pltpu.VMEM((n, heads, pages, HD), jnp.bfloat16),
            pltpu.VMEM((n, 2 * heads, PAGE), jnp.float32),
            pltpu.VMEM((heads, reqs, HD), jnp.bfloat16),
            pltpu.VMEM((blocks, merged, block), jnp.float32),
            pltpu.VMEM(out_proj.shape, jnp.bfloat16),
            pltpu.VMEM((groups, merged, heads // groups * HD), jnp.bfloat16),
            dma((10,)),
            dma((back // 2, groups, 2, CUTS)),
            dma((back // 2, groups, 2, CUTS)),
            dma((back // 2, groups, 2, CUTS)),
            dma((back // 2, groups, 2, CUTS)),
            dma((groups + 1,)),
            dma((n, groups + 1)),
            dma((n // 2, groups)),
            dma((2, groups)),
            dma((groups,)),
            dma((groups,)),
            dma((groups,)),
            dma((groups,)),
            pltpu.SemaphoreType.REGULAR,
        ],
        compiler_params=pltpu.CompilerParams(
            collective_id=0, has_side_effects=True, vmem_limit_bytes=48 * 1024 * 1024
        ),
    )(*[pltpu.with_memory_space_constraint(x, pltpu.HBM) for x in args])
    return pl.pallas_call(
        put,
        out_shape=tuple(jax.ShapeDtypeStruct(x.shape, x.dtype) for x in result),
        in_specs=[vmem, vmem],
        out_specs=(hbm, hbm),
        scratch_shapes=[dma((2,))],
        compiler_params=pltpu.CompilerParams(vmem_limit_bytes=4 * 1024 * 1024),
    )(*result)


def solution(mesh):
    placed = (
        P(("rep", "seq"), "tp"),
        P(("rep", "seq"), "tp"),
        P(("rep", "seq"), "tp"),
        P("rep"),
        P("tp"),
        P("rep", "tp"),
        P("rep", "tp"),
        P("rep", "tp"),
        P(("rep", "seq"), "tp"),
        P(("rep", "seq"), "tp"),
        P(("rep", "seq")),
        P("rep"),
        P("tp", None),
    )
    return jax.shard_map(
        functools.partial(on_device, mesh.shape["seq"]),
        mesh=mesh,
        in_specs=placed,
        out_specs=(P(("rep", "seq", "tp"), None), P(("rep", "tp"), None)),
        check_vma=False,
    )
```
